32 devices in a mesh: leaf: 32 (over z, y, x, core).
Axes of the slice: x: 2, y: 2, z: 4, core: 2. Of those that a mesh axis runs over, the one named last changes fastest.
Arguments:
- right_side: float32 [32768, 128], P('leaf'), may hold values from -6 to 6
- diag_blocks: bfloat16 [32, 1024, 1024], P('leaf'), may hold values from -0.1875 to 0.1875
- row_bases: bfloat16 [32, 200, 1024], P('leaf'), may hold values from -0.4375 to 0.4375
- column_bases: bfloat16 [32, 200, 1024], P('leaf'), may hold values from -0.1875 to 0.1875
- transfer: bfloat16 [5, 2, 200, 200], replicated, may hold values from -0.375 to 0.375
- coupling: bfloat16 [5, 2, 200, 200], replicated, may hold values from -0.4375 to 0.4375
- inverse_blocks: bfloat16 [32, 1024, 1024], P('leaf'), may hold values from -0.1875 to 0.1875
- inverse_rows: bfloat16 [32, 200, 1024], P('leaf'), may hold values from -0.4375 to 0.4375
- inverse_columns: bfloat16 [32, 200, 1024], P('leaf'), may hold values from -0.1875 to 0.1875
- inverse_transfer: bfloat16 [5, 2, 200, 200], replicated, may hold values from -0.375 to 0.375
- inverse_coupling: bfloat16 [5, 2, 200, 200], replicated, may hold values from -0.4375 to 0.4375
Outputs:
- solution: float32 [32768, 128], P('leaf')
- hessenberg: float32 [4, 3, 128], replicated
The draws below stay inside these ranges and needn't reach their ends.
All inputs are finite; a program needn't handle non-finite values.
Results may differ from the reference program's by a relative error of at most 0.0003.
Values sent between devices are 32-bit elements; how exact they have to be, the bound alone decides.
No kernel may reach another device: no remote copies, remote signals or barrier semaphores. Data moves between devices by JAX's collectives and lax.ppermute only.
A program may use at most 128 MiB of HBM per device.

```python
import jax
import jax.numpy as jnp
from jax import lax

LEAF = 1024
K = 200
NRHS = 128
ITERS = 3
LEVELS = 5
ORDER = 32768
N_LEAF = 32


def block_levels(key, dims, shards, smallest, high):
    def one(position, blocks):
        draws = jax.random.uniform(jax.random.fold_in(jax.random.fold_in(key, 6), position), (blocks,), jnp.float32, smallest / len(shards), high / len(shards))
        return jnp.repeat(jnp.exp(draws), dims[position] // blocks).reshape((-1,) + (1,) * (len(dims) - position - 1))

    level = one(*shards[0])
    for cut in shards[1:]:
        level = level * one(*cut)
    return level


def centred(rng, extent, scale, limit, shards=(), held_as=jnp.bfloat16):
    gain = block_levels(rng, extent, shards, -0.22, 0.18) if shards else 1.0
    result = jax.random.normal(rng, extent, jnp.float32) * scale * gain
    return jnp.minimum(jnp.maximum(result, -limit), limit).astype(held_as)


def setup_inputs(seed: int = 0) -> dict:
    splits = jax.random.split(jax.random.key(seed), 12)
    return {
        "right_side": centred(splits[0], (ORDER, NRHS), 1.0, 6.0, ((0, 32),), jnp.float32),
        "diag_blocks": centred(splits[1], (N_LEAF, LEAF, LEAF), LEAF ** -0.5, 0.1875, ((0, 32),)),
        "row_bases": centred(splits[2], (N_LEAF, K, LEAF), K ** -0.5, 0.4375, ((0, 32),)),
        "column_bases": centred(splits[3], (N_LEAF, K, LEAF), LEAF ** -0.5, 0.1875, ((0, 32),)),
        "transfer": centred(splits[4], (LEVELS, 2, K, K), (K * 7 // 5) ** -0.5, 0.375),
        "coupling": centred(splits[5], (LEVELS, 2, K, K), K ** -0.5, 0.4375),
        "inverse_blocks": centred(splits[6], (N_LEAF, LEAF, LEAF), LEAF ** -0.5, 0.1875, ((0, 32),)),
        "inverse_rows": centred(splits[7], (N_LEAF, K, LEAF), K ** -0.5, 0.4375, ((0, 32),)),
        "inverse_columns": centred(splits[8], (N_LEAF, K, LEAF), LEAF ** -0.5, 0.1875, ((0, 32),)),
        "inverse_transfer": centred(splits[9], (LEVELS, 2, K, K), (K * 7 // 5) ** -0.5, 0.375),
        "inverse_coupling": centred(splits[10], (LEVELS, 2, K, K), K ** -0.5, 0.4375),
    }


EPSILON = 1e-06

def transpose_apply(matrix, vectors):
    return lax.dot_general(matrix, vectors, (((0,), (0,)), ((), ())), precision=lax.Precision.HIGHEST)

def hss_apply(vectors, blocks, row_side, column_side, transfer, coupling):
    leaves = blocks.shape[0]
    leaf_width = blocks.shape[1]
    basis_rank = transfer.shape[2]
    columns = vectors.shape[1]
    levels = transfer.shape[0]
    pieces = vectors.reshape(leaves, leaf_width, columns)

    def leaf_terms(bundle):
        square, column_base, portion = bundle
        direct = jnp.dot(square.astype(jnp.float32), portion, precision=lax.Precision.HIGHEST)
        summary = jnp.dot(column_base.astype(jnp.float32), portion, precision=lax.Precision.HIGHEST)
        return (direct, summary)
    direct, summary = lax.map(leaf_terms, (blocks, column_side, pieces))
    siblings = []
    for height in range(levels):
        paired = summary.reshape(-1, 2, basis_rank, columns)
        siblings.append(paired[:, ::-1])
        if height < levels - 1:
            translate = transfer[height].astype(jnp.float32)
            summary = jnp.einsum('ij,nir->njr', translate[0], paired[:, 0], precision=lax.Precision.HIGHEST) + jnp.einsum('ij,nir->njr', translate[1], paired[:, 1], precision=lax.Precision.HIGHEST)
    downward = None
    for height in reversed(range(levels)):
        bridge = coupling[height].astype(jnp.float32)
        incoming = jnp.einsum('sij,psjr->psir', bridge, siblings[height], precision=lax.Precision.HIGHEST)
        if downward is not None:
            translate = transfer[height].astype(jnp.float32)
            incoming = incoming + jnp.einsum('sij,pjr->psir', translate, downward, precision=lax.Precision.HIGHEST)
        downward = incoming.reshape(-1, basis_rank, columns)

    def leaf_out(bundle):
        row_base, portion = bundle
        return transpose_apply(row_base.astype(jnp.float32), portion)
    spread = lax.map(leaf_out, (row_side, downward))
    return (direct + spread).reshape(leaves * leaf_width, columns)

def least_squares(entries, beta_first):
    unknowns = len(entries[0])
    matrix = [list(line) for line in entries]
    target = [beta_first] + [jnp.zeros_like(beta_first) for column in range(unknowns)]
    for column in range(unknowns):
        upper_entry = matrix[column][column]
        lower_entry = matrix[column + 1][column]
        radius = jnp.sqrt(upper_entry * upper_entry + lower_entry * lower_entry)
        cosine = upper_entry / radius
        sine_value = lower_entry / radius
        for following in range(column, unknowns):
            top_value = matrix[column][following]
            bottom_value = matrix[column + 1][following]
            matrix[column][following] = cosine * top_value + sine_value * bottom_value
            matrix[column + 1][following] = cosine * bottom_value - sine_value * top_value
        top_value = target[column]
        bottom_value = target[column + 1]
        target[column] = cosine * top_value + sine_value * bottom_value
        target[column + 1] = cosine * bottom_value - sine_value * top_value
    coefficients = [None] * unknowns
    for current_row in reversed(range(unknowns)):
        remainder = target[current_row]
        for following in range(current_row + 1, unknowns):
            remainder = remainder - matrix[current_row][following] * coefficients[following]
        coefficients[current_row] = remainder / matrix[current_row][current_row]
    return coefficients

def reference(right_side, diag_blocks, row_bases, column_bases, transfer, coupling, inverse_blocks, inverse_rows, inverse_columns, inverse_transfer, inverse_coupling):
    beta_first = jnp.sqrt(lax.optimization_barrier(jnp.sum(right_side * right_side, axis=0)) + EPSILON)
    krylov = [right_side / beta_first]
    images = []
    zero_row = jnp.zeros_like(beta_first)
    entries = [[zero_row for column in range(ITERS)] for line in range(ITERS + 1)]
    for column in range(ITERS):
        image = hss_apply(krylov[column], inverse_blocks, inverse_rows, inverse_columns, inverse_transfer, inverse_coupling)
        images.append(image)
        mixed = hss_apply(image, diag_blocks, row_bases, column_bases, transfer, coupling)
        correction = jnp.zeros_like(mixed)
        for earlier in range(column + 1):
            product = lax.optimization_barrier(jnp.sum(krylov[earlier] * mixed, axis=0))
            entries[earlier][column] = product
            correction = correction + product * krylov[earlier]
        update = mixed - correction
        norm_value = jnp.sqrt(lax.optimization_barrier(jnp.sum(update * update, axis=0)) + EPSILON)
        entries[column + 1][column] = norm_value
        krylov.append(update / norm_value)
    coefficients = least_squares(entries, beta_first)
    solution = jnp.zeros_like(right_side)
    for column in range(ITERS):
        solution = solution + coefficients[column] * images[column]
    hessenberg = jnp.stack([jnp.stack(line) for line in entries])
    return (solution, hessenberg)
```

```python
import jax
import jax.numpy as jnp
from jax import lax
from jax.sharding import PartitionSpec as P

ITERS = 3
EPSILON = 1e-06
SUMS = 8


def from_partner(block, mask):
    count = lax.axis_size("leaf")
    return lax.ppermute(block, "leaf", [(i, i ^ mask) for i in range(count)])


def split3(x):
    high = lax.reduce_precision(x, 8, 7)
    rest = x - high
    middle = lax.reduce_precision(rest, 8, 7)
    low = rest - middle
    return jnp.concatenate([high, middle, low], axis=1).astype(jnp.bfloat16)


def product(matrix, x, contract):
    n = x.shape[1]
    y = lax.dot_general(
        matrix, split3(x), (((contract,), (0,)), ((), ())), preferred_element_type=jnp.float32
    )
    return y[:, :n] + (y[:, n : 2 * n] + y[:, 2 * n :])


def mm(matrix, x):
    return product(matrix, x, 1)


def mmt(matrix, x):
    return product(matrix, x, 0)


def pack(c, sums):
    full = jnp.concatenate([c, sums], axis=0)
    rows = full.shape[0] // 2
    return jnp.concatenate([full[:rows], full[rows:]], axis=1)


def unpack(packed):
    half = packed.shape[1] // 2
    full = jnp.concatenate([packed[:, :half], packed[:, half:]], axis=0)
    return full[:-SUMS], full[-SUMS:]


def swap_leaf(matrix):
    got = from_partner(matrix.astype(jnp.float32), 1)
    one = 1.0 + jnp.minimum(lax.axis_index("leaf"), 0).astype(jnp.float32)
    return (got * one).astype(jnp.bfloat16)


def pick(pairs, side):
    return lax.dynamic_index_in_dim(pairs, side, 0, keepdims=False)


class Operator:
    def __init__(self, blocks, rows, columns, transfer, coupling):
        position = lax.axis_index("leaf")
        levels = transfer.shape[0]
        self.levels = levels
        self.columns = (columns[0], swap_leaf(columns[0]))
        self.blocks = (blocks[0], swap_leaf(blocks[0]))
        self.rows = (rows[0], swap_leaf(rows[0]))
        side = [position >> h & 1 for h in range(levels)]
        self.up = [
            (pick(transfer[h], side[h]), pick(transfer[h], 1 - side[h])) for h in range(levels)
        ]
        self.cross = [
            (pick(coupling[h], side[h]), pick(coupling[h], 1 - side[h])) for h in range(levels)
        ]

    def apply(self, v, sums):
        half = v.shape[1] // 2
        levels = self.levels
        own, near = v[:, :half], v[:, half:]
        c_own, c_near = mm(self.columns[0], own), mm(self.columns[1], near)
        siblings = [None] * levels
        c = None
        if levels > 1:
            c = mmt(self.up[0][0], c_own) + mmt(self.up[0][1], c_near)
        h = 1
        while h < levels:
            sent = pack(c, sums)
            last = h + 1 == levels
            siblings[h], s_a = unpack(from_partner(sent, 1 << h))
            if last:
                sums = sums + s_a
                break
            c_b, s_b = unpack(from_partner(sent, 2 << h))
            c_ab, s_ab = unpack(from_partner(sent, 3 << h))
            sums = (sums + s_a) + (s_b + s_ab)
            both = mmt(self.up[h][0], jnp.concatenate([c, c_b], 1)) + mmt(
                self.up[h][1], jnp.concatenate([siblings[h], c_ab], 1)
            )
            siblings[h + 1] = both[:, half:]
            if h + 2 < levels:
                c = mmt(self.up[h + 1][0], both[:, :half]) + mmt(
                    self.up[h + 1][1], siblings[h + 1]
                )
            h += 2
        d = None
        for h in reversed(range(1, levels)):
            incoming = mm(self.cross[h][0], siblings[h])
            d = incoming if d is None else incoming + mm(self.up[h][0], d)
        d_own, d_near = mm(self.cross[0][0], c_near), mm(self.cross[0][1], c_own)
        if d is not None:
            d_own = d_own + mm(self.up[0][0], d)
            d_near = d_near + mm(self.up[0][1], d)
        out_own = mm(self.blocks[0], own) + mmt(self.rows[0], d_own)
        out_near = mm(self.blocks[1], near) + mmt(self.rows[1], d_near)
        return jnp.concatenate([out_own, out_near], 1), sums


def least_squares(entries, beta_first):
    unknowns = len(entries[0])
    matrix = [list(line) for line in entries]
    target = [beta_first] + [jnp.zeros_like(beta_first) for column in range(unknowns)]
    for column in range(unknowns):
        upper_entry = matrix[column][column]
        lower_entry = matrix[column + 1][column]
        radius = jnp.sqrt(upper_entry * upper_entry + lower_entry * lower_entry)
        cosine = upper_entry / radius
        sine_value = lower_entry / radius
        for following in range(column, unknowns):
            top_value = matrix[column][following]
            bottom_value = matrix[column + 1][following]
            matrix[column][following] = cosine * top_value + sine_value * bottom_value
            matrix[column + 1][following] = cosine * bottom_value - sine_value * top_value
        top_value = target[column]
        bottom_value = target[column + 1]
        target[column] = cosine * top_value + sine_value * bottom_value
        target[column + 1] = cosine * bottom_value - sine_value * top_value
    coefficients = [None] * unknowns
    for current_row in reversed(range(unknowns)):
        remainder = target[current_row]
        for following in range(current_row + 1, unknowns):
            remainder = remainder - matrix[current_row][following] * coefficients[following]
        coefficients[current_row] = remainder / matrix[current_row][current_row]
    return coefficients


def partials(products):
    rows = [jnp.sum(p, axis=0) for p in products]
    half = rows[0].shape[0] // 2
    rows = [r[:half] + r[half:] for r in rows]
    rows = rows + [jnp.zeros_like(rows[0])] * (SUMS - len(rows))
    return jnp.stack(rows)


def everywhere(sums):
    count = lax.axis_size("leaf")
    sent = jnp.broadcast_to(sums[None], (count,) + sums.shape)
    got = lax.all_to_all(sent, "leaf", 0, 0)
    return jnp.sum(got.reshape((count // 2, 2) + sums.shape), axis=0)


def twice(row):
    return jnp.concatenate([row, row])


def on_device(
    right_side,
    diag_blocks,
    row_bases,
    column_bases,
    transfer,
    coupling,
    inverse_blocks,
    inverse_rows,
    inverse_columns,
    inverse_transfer,
    inverse_coupling,
):
    side = lax.axis_index("leaf") & 1
    half = right_side.shape[1] // 2
    low, high = right_side[:, :half], right_side[:, half:]
    kept = jnp.where(side == 0, low, high)
    given = from_partner(jnp.where(side == 0, high, low), 1)
    r = jnp.concatenate([kept, given], 1)
    inverse = Operator(
        inverse_blocks, inverse_rows, inverse_columns, inverse_transfer, inverse_coupling
    )
    forward = Operator(diag_blocks, row_bases, column_bases, transfer, coupling)

    zero = jnp.zeros((half,), jnp.float32)
    entries = [[zero] * ITERS for line in range(ITERS + 1)]
    raw, totals = inverse.apply(r, partials([r * r]))
    beta_first = jnp.sqrt(totals[0] + EPSILON)
    krylov = [r / twice(beta_first)]
    images = [raw / twice(beta_first)]
    w, _ = forward.apply(images[0], partials([jnp.zeros_like(r)]))
    for column in range(ITERS - 1):
        raw, totals = inverse.apply(w, partials([q * w for q in krylov]))
        u, image = w, raw
        for i in range(column + 1):
            entries[i][column] = totals[i]
            u = u - twice(totals[i]) * krylov[i]
            image = image - twice(totals[i]) * images[i]
        w, totals = forward.apply(image, partials([u * u]))
        norm = jnp.sqrt(totals[0] + EPSILON)
        entries[column + 1][column] = norm
        krylov.append(u / twice(norm))
        images.append(image / twice(norm))
        w = w / twice(norm)
    last = ITERS - 1
    side_totals = everywhere(partials([q * w for q in krylov]))
    mine = lax.dynamic_index_in_dim(side_totals, side, 0, keepdims=False)
    u = w
    for i in range(ITERS):
        entries[i][last] = mine[i]
        u = u - twice(mine[i]) * krylov[i]
    side_totals = everywhere(partials([u * u]))
    mine = lax.dynamic_index_in_dim(side_totals, side, 0, keepdims=False)
    entries[ITERS][last] = jnp.sqrt(mine[0] + EPSILON)
    y = least_squares(entries, beta_first)
    x = jnp.zeros_like(r)
    for i in range(ITERS):
        x = x + twice(y[i]) * images[i]
    hess = jnp.stack([jnp.stack(line) for line in entries])
    x_near = from_partner(x[:, half:], 1)
    hess_near = from_partner(hess, 1)
    x_own = x[:, :half]
    solution = jnp.where(
        side == 0, jnp.concatenate([x_own, x_near], 1), jnp.concatenate([x_near, x_own], 1)
    )
    hess = jnp.where(
        side == 0, jnp.concatenate([hess, hess_near], 2), jnp.concatenate([hess_near, hess], 2)
    )
    return (solution, hess)


def solution(mesh):
    in_specs = (
        P("leaf", None),
        P("leaf", None, None),
        P("leaf", None, None),
        P("leaf", None, None),
        P(),
        P(),
        P("leaf", None, None),
        P("leaf", None, None),
        P("leaf", None, None),
        P(),
        P(),
    )
    out_specs = (P("leaf", None), P())
    return jax.shard_map(
        on_device, mesh=mesh, in_specs=in_specs, out_specs=out_specs, check_vma=False
    )
```

```python
import functools

import jax
import jax.numpy as jnp
from jax import lax
from jax.experimental import pallas as pl
from jax.experimental.pallas import tpu as pltpu
from jax.sharding import PartitionSpec as P

ITERS = 3
EPSILON = 1e-06
SUMS = 8
F32 = jnp.float32
BF16 = jnp.bfloat16


def from_partner(block, mask):
    count = lax.axis_size("leaf")
    return lax.ppermute(block, "leaf", [(i, i ^ mask) for i in range(count)])


def shape(*dims, dtype=F32):
    return jax.ShapeDtypeStruct(dims, dtype)


def call(kernel, out, name, flops, *args):
    return pl.pallas_call(
        kernel,
        out_shape=out,
        name=name,
        cost_estimate=pl.CostEstimate(flops=flops, bytes_accessed=flops // 512, transcendentals=0),
    )(*args)


def split3(x):
    high = x.astype(BF16)
    rest = x - high.astype(F32)
    middle = rest.astype(BF16)
    low = (rest - middle.astype(F32)).astype(BF16)
    return jnp.concatenate([high, middle, low], axis=0)


def times(x, matrix, contract):
    n = x.shape[0]
    y = lax.dot_general(
        split3(x), matrix, (((1,), (contract,)), ((), ())), preferred_element_type=F32
    )
    return y[:n] + (y[n : 2 * n] + y[2 * n :])


def nn(x, matrix):
    return times(x, matrix, 0)


def nt(x, matrix):
    return times(x, matrix, 1)


def side_of(height):
    return lax.axis_index("leaf") >> height & 1


def join(c, sums, width):
    if c is None:
        n, rank = sums[0].shape[0], 0
        block = jnp.zeros((n, width), F32)
    else:
        n, rank = c.shape
        block = jnp.concatenate([c, jnp.zeros((n, width - rank), F32)], axis=1)
    lane = lax.broadcasted_iota(jnp.int32, (n, width), 1)
    for i, s in enumerate(sums):
        block = jnp.where(lane == rank + i, s, block)
    return block


def first_kernel(r_ref, columns_ref, kept_ref, sent_ref, r_kept_ref, r_sent_ref):
    rt = jnp.transpose(r_ref[...])
    half = rt.shape[0] // 2
    full = join(
        nt(rt, columns_ref[0]), [jnp.sum(rt * rt, axis=1, keepdims=True)], kept_ref.shape[1]
    )
    even = side_of(0) == 0
    kept_ref[...] = jnp.where(even, full[:half], full[half:])
    sent_ref[...] = jnp.where(even, full[half:], full[:half])
    r_kept_ref[...] = jnp.where(even, rt[:half], rt[half:])
    r_sent_ref[...] = jnp.where(even, rt[half:], rt[:half])


def meet_kernel(kept_ref, got_ref, transfer_ref, out_ref):
    rank = transfer_ref.shape[2]
    side = side_of(0)
    c = nn(kept_ref[:, :rank], transfer_ref[0, side])
    c = c + nn(got_ref[:, :rank], transfer_ref[0, 1 - side])
    sums = kept_ref[:, rank:] + got_ref[:, rank:]
    out_ref[...] = jnp.concatenate([c, sums], axis=1)


def total(own, received, rank):
    sums = [x[:, rank:] for x in [own] + received]
    if len(sums) == 2:
        return sums[0] + sums[1]
    return (sums[0] + sums[1]) + (sums[2] + sums[3])


def climb(own, received, rank, height, transfer_ref):
    side = side_of(height)
    first, second, third = received
    even = jnp.concatenate([own[:, :rank], second[:, :rank]], axis=0)
    odd = jnp.concatenate([first[:, :rank], third[:, :rank]], axis=0)
    return nn(even, transfer_ref[height, side]) + nn(odd, transfer_ref[height, 1 - side])


def middle_kernel(height, own_ref, a_ref, b_ref, ab_ref, transfer_ref, out_ref, sibling_ref):
    rank = transfer_ref.shape[2]
    own, received = own_ref[...], [a_ref[...], b_ref[...], ab_ref[...]]
    n = own.shape[0]
    both = climb(own, received, rank, height, transfer_ref)
    side = side_of(height + 1)
    c = nn(both[:n], transfer_ref[height + 1, side])
    c = c + nn(both[n:], transfer_ref[height + 1, 1 - side])
    out_ref[...] = jnp.concatenate([c, total(own, received, rank)], axis=1)
    sibling_ref[...] = both[n:]


def cross_kernel(own_ref, near_ref, *refs):
    *siblings, coupling_ref, out_ref = refs
    rank = coupling_ref.shape[2]
    side = side_of(0)
    out_ref[0] = nt(near_ref[:, :rank], coupling_ref[0, side])
    out_ref[1] = nt(own_ref[:, :rank], coupling_ref[0, 1 - side])
    for i, sibling in enumerate(siblings):
        h = i + 1
        out_ref[h + 1] = nt(sibling[:, :rank], coupling_ref[h, side_of(h)])


def block_kernel(v_ref, own_ref, near_ref, out_ref):
    out_ref[0] = nt(v_ref[0], own_ref[...])
    out_ref[1] = nt(v_ref[1], near_ref[...])


def widen_kernel(x_ref, out_ref):
    out_ref[...] = x_ref[0].astype(F32)


def narrow_kernel(x_ref, out_ref):
    out_ref[...] = x_ref[...].astype(BF16)


def swapped(matrix):
    rows, columns = matrix.shape[1:]
    wide = call(widen_kernel, shape(rows, columns), "widen", rows * columns, matrix)
    wide = from_partner(wide, 1)
    return call(narrow_kernel, shape(rows, columns, dtype=BF16), "narrow", rows * columns, wide)


def descend(heights, own, received, cross, transfer_ref, coupling_ref):
    rank = transfer_ref.shape[2]
    low = heights[0]
    side = side_of(low)
    d = nt(received[0][:, :rank], coupling_ref[low, side])
    if len(heights) == 2:
        high = heights[1]
        even, odd = received[1][:, :rank], received[2][:, :rank]
        sibling = nn(even, transfer_ref[low, side]) + nn(odd, transfer_ref[low, 1 - side])
        top = nt(sibling, coupling_ref[high, side_of(high)])
        d = d + nt(top, transfer_ref[low, side])
    for h in reversed(range(1, low)):
        d = cross[h + 1] + nt(d, transfer_ref[h, side_of(h)])
    side = side_of(0)
    d_own = cross[0] + nt(d, transfer_ref[0, side])
    d_near = cross[1] + nt(d, transfer_ref[0, 1 - side])
    return d_own, d_near


def spread(refs, heights, d_refs):
    own, received, cross, blocks, rows_own, rows_near, transfer_ref, coupling_ref = refs
    d_own, d_near = descend(heights, own, received, cross, transfer_ref, coupling_ref)
    return blocks[0] + nn(d_own, rows_own), blocks[1] + nn(d_near, rows_near)


def column_sum(x, y):
    return jnp.sum(x[0] * y[0], axis=1, keepdims=True) + jnp.sum(
        x[1] * y[1], axis=1, keepdims=True
    )


def send_off(v, sums, columns_own, columns_near, transfer_ref, own_ref, near_ref, out_ref):
    rank = transfer_ref.shape[2]
    width = out_ref.shape[1]
    c_own, c_near = nt(v[0], columns_own), nt(v[1], columns_near)
    side = side_of(0)
    c = nn(c_own, transfer_ref[0, side]) + nn(c_near, transfer_ref[0, 1 - side])
    own_ref[...] = c_own
    near_ref[...] = c_near
    out_ref[...] = join(c, sums, width)


def read(refs, received_count):
    own = refs[0][...]
    received = [r[...] for r in refs[1 : 1 + received_count]]
    cross, blocks, rows_own, rows_near, transfer, coupling = refs[
        1 + received_count : 7 + received_count
    ]
    rank = transfer.shape[2]
    values = (own, received, cross, blocks, rows_own[0], rows_near[...], transfer, coupling)
    return values, total(own, received, rank), refs[7 + received_count :]


def inverse_end_kernel(column, heights, count, *refs):
    values, totals, rest = read(refs, count)
    columns_own, columns_near, transfer_next, *rest = rest
    w = rest[0]
    krylov = rest[1 : 1 + column]
    images = rest[1 + column : 1 + 2 * column]
    u_ref, z_ref, totals_ref, own_ref, near_ref, out_ref = rest[1 + 2 * column :]
    raw = spread(values, heights, None)
    totals_ref[...] = totals
    u, z = [w[0], w[1]], list(raw)
    if column == 0:
        norm = jnp.sqrt(totals[:, 0:1] + EPSILON)
        u = [x / norm for x in u]
        z = [x / norm for x in z]
        sums = []
    else:
        for i in range(column):
            h = totals[:, i : i + 1]
            for side in range(2):
                u[side] = u[side] - h * krylov[i][side]
                z[side] = z[side] - h * images[i][side]
        sums = [column_sum(u, u)]
    for side in range(2):
        u_ref[side] = u[side]
        z_ref[side] = z[side]
    send_off(z, sums, columns_own[0], columns_near[...], transfer_next, own_ref, near_ref, out_ref)


def forward_end_kernel(column, last, heights, count, *refs):
    values, totals, rest = read(refs, count)
    if not last:
        columns_own, columns_near, transfer_next, *rest = rest
    raw = spread(values, heights, None)
    w = list(raw)
    earlier = rest[:column]
    rest = rest[column:]
    if column == 0:
        u_ref, *rest = rest
        q = [u_ref[0], u_ref[1]]
    else:
        u_ref, z_ref, q_ref, z_out_ref, totals_ref, *rest = rest
        totals_ref[...] = totals
        norm = jnp.sqrt(totals[:, 0:1] + EPSILON)
        q = [u_ref[side] / norm for side in range(2)]
        w = [x / norm for x in w]
        for side in range(2):
            q_ref[side] = q[side]
            z_out_ref[side] = z_ref[side] / norm
    sums = [column_sum(x, w) for x in list(earlier) + [q]]
    w_ref, *rest = rest
    for side in range(2):
        w_ref[side] = w[side]
    if last:
        block = join(None, sums, 128)
        rest[0][...] = jnp.transpose(block)[:SUMS]
    else:
        own_ref, near_ref, out_ref = rest
        send_off(
            w, sums, columns_own[0], columns_near[...], transfer_next, own_ref, near_ref, out_ref
        )


def gathered(got_ref, side):
    parts = [got_ref[i] for i in range(got_ref.shape[0])]
    while len(parts) > 2:
        parts = [
            parts[4 * (i // 2) + i % 2] + parts[4 * (i // 2) + 2 + i % 2]
            for i in range(len(parts) // 2)
        ]
    return jnp.where(side == 0, parts[0], parts[1])


def columns_of(rows):
    n = rows.shape[1]
    padded = jnp.concatenate([rows, jnp.zeros((128 - rows.shape[0], n), F32)], axis=0)
    return jnp.transpose(padded)


def closing_kernel(got_ref, q0_ref, q1_ref, q2_ref, w_ref, rows_ref, out_ref):
    rows = gathered(got_ref, side_of(0))
    rows_ref[...] = rows
    h = columns_of(rows)
    u = [w_ref[0], w_ref[1]]
    for i, q in enumerate([q0_ref, q1_ref, q2_ref]):
        for side in range(2):
            u[side] = u[side] - h[:, i : i + 1] * q[side]
    block = join(None, [column_sum(u, u)], 128)
    out_ref[...] = jnp.transpose(block)[:SUMS]


def least_squares(entries, beta_first):
    unknowns = len(entries[0])
    matrix = [list(line) for line in entries]
    target = [beta_first] + [jnp.zeros_like(beta_first) for column in range(unknowns)]
    for column in range(unknowns):
        upper_entry = matrix[column][column]
        lower_entry = matrix[column + 1][column]
        radius = jnp.sqrt(upper_entry * upper_entry + lower_entry * lower_entry)
        cosine = upper_entry / radius
        sine_value = lower_entry / radius
        for following in range(column, unknowns):
            top_value = matrix[column][following]
            bottom_value = matrix[column + 1][following]
            matrix[column][following] = cosine * top_value + sine_value * bottom_value
            matrix[column + 1][following] = cosine * bottom_value - sine_value * top_value
        top_value = target[column]
        bottom_value = target[column + 1]
        target[column] = cosine * top_value + sine_value * bottom_value
        target[column + 1] = cosine * bottom_value - sine_value * top_value
    coefficients = [None] * unknowns
    for current_row in reversed(range(unknowns)):
        remainder = target[current_row]
        for following in range(current_row + 1, unknowns):
            remainder = remainder - matrix[current_row][following] * coefficients[following]
        coefficients[current_row] = remainder / matrix[current_row][current_row]
    return coefficients


def answer_kernel(got_ref, rows_ref, *refs):
    totals, (z0, z1, z2, x_own_ref, x_near_ref, hess_ref) = refs[:5], refs[5:]
    width = totals[0].shape[1]

    def rows_of(ref):
        block = ref[...]
        if width < 128:
            block = jnp.concatenate([block, jnp.zeros((block.shape[0], 128 - width), F32)], 1)
        return jnp.transpose(block)

    beta_row, h0, n0, h1, n1 = [rows_of(t) for t in totals]
    square = gathered(got_ref, side_of(0))
    rows = rows_ref[...]

    def root(x):
        return jnp.sqrt(x[0:1] + EPSILON)

    beta = root(beta_row)
    zero = jnp.zeros_like(beta)
    entries = [
        [h0[0:1], h1[0:1], rows[0:1]],
        [root(n0), h1[1:2], rows[1:2]],
        [zero, root(n1), rows[2:3]],
        [zero, zero, root(square)],
    ]
    y = least_squares(entries, beta)
    y = columns_of(jnp.concatenate(y, axis=0))
    for side, out in enumerate([x_own_ref, x_near_ref]):
        out[...] = (
            y[:, 0:1] * z0[side] + y[:, 1:2] * z1[side] + y[:, 2:3] * z2[side]
        )
    hess_ref[...] = jnp.concatenate([e for line in entries for e in line], axis=0)


def finish_kernel(x_ref, got_ref, hess_ref, hess_got_ref, out_ref, hess_out_ref):
    even = side_of(0) == 0
    own, got = x_ref[...], got_ref[...]
    out_ref[...] = jnp.transpose(
        jnp.concatenate([jnp.where(even, own, got), jnp.where(even, got, own)], axis=0)
    )
    own, got = hess_ref[...], hess_got_ref[...]
    hess_out_ref[...] = jnp.concatenate(
        [jnp.where(even, own, got), jnp.where(even, got, own)], axis=1
    )


class Operator:
    def __init__(self, blocks, rows, columns, transfer, coupling):
        self.blocks, self.rows, self.columns = blocks, rows, columns
        self.transfer, self.coupling = transfer, coupling
        self.near = {}

    def fetch(self, name):
        if name not in self.near:
            self.near[name] = swapped(getattr(self, name))
        return getattr(self, name), self.near[name]


def exchange(block, height, levels):
    masks = [1 << height]
    if height + 1 < levels:
        masks += [2 << height, 3 << height]
    return [from_partner(block, mask) for mask in masks]


def rounds(op, block, own, near):
    levels, _, rank, _ = op.transfer.shape
    n, width = block.shape
    siblings = []
    h = 1
    unit = 6 * n * rank * rank
    while h + 2 < levels:
        received = exchange(block, h, levels)
        siblings.append(received[0])
        block, sibling = call(
            functools.partial(middle_kernel, h),
            (shape(n, width), shape(n, rank)),
            "middle",
            6 * unit,
            block,
            *received,
            op.transfer,
        )
        siblings.append(sibling)
        h += 2
    heights = tuple(range(h, levels))
    received = exchange(block, h, levels)
    cross = call(
        cross_kernel,
        shape(h + 1, n, rank),
        "cross",
        (h + 1) * unit,
        own,
        near,
        *siblings,
        op.coupling,
    )
    return heights, block, received, cross


def on_device(
    right_side,
    diag_blocks,
    row_bases,
    column_bases,
    transfer,
    coupling,
    inverse_blocks,
    inverse_rows,
    inverse_columns,
    inverse_transfer,
    inverse_coupling,
):
    inverse = Operator(
        inverse_blocks, inverse_rows, inverse_columns, inverse_transfer, inverse_coupling
    )
    forward = Operator(diag_blocks, row_bases, column_bases, transfer, coupling)
    leaf, columns = right_side.shape
    n = columns // 2
    rank = transfer.shape[2]
    width = -(-(rank + SUMS) // 128) * 128
    unit = 6 * n * rank * rank
    big = 6 * n * rank * leaf

    kept, sent, r_kept, r_sent = call(
        first_kernel,
        (shape(n, width), shape(n, width), shape(n, leaf), shape(n, leaf)),
        "first",
        big,
        right_side,
        inverse_columns,
    )
    got = from_partner(sent, 1)
    block = call(meet_kernel, shape(n, width), "meet", 2 * unit, kept, got, inverse_transfer)
    own, near = kept, got
    r_got = from_partner(r_sent, 1)
    w = jnp.stack([r_kept, r_got])

    def finish_operands(op, state, v):
        heights, block, received, cross = state
        e_own, e_near = op.fetch("blocks")
        product = call(
            block_kernel,
            shape(2, n, leaf),
            "blocks",
            12 * n * leaf * leaf,
            v,
            e_own[0],
            e_near,
        )
        p_own, p_near = op.fetch("rows")
        return heights, (block, *received, cross, product, p_own, p_near, op.transfer, op.coupling)

    def vectors():
        return shape(2, n, leaf)

    tail = (shape(n, rank), shape(n, rank), shape(n, width))
    sums_shape = shape(n, width - rank)
    krylov, images, totals = [], [], []
    for column in range(ITERS):
        last = column + 1 == ITERS
        state = rounds(inverse, block, own, near)
        heights, operands = finish_operands(inverse, state, w)
        u, z, t, own, near, block = call(
            functools.partial(inverse_end_kernel, column, heights, len(state[2])),
            (vectors(), vectors(), sums_shape) + tail,
            "inverse_end",
            4 * big,
            *operands,
            *forward.fetch("columns"),
            forward.transfer,
            w,
            *krylov,
            *images,
        )
        totals.append(t)
        state = rounds(forward, block, own, near)
        heights, operands = finish_operands(forward, state, z)
        extra = [] if last else [*inverse.fetch("columns"), inverse.transfer]
        out = [vectors()] if column == 0 else [vectors(), vectors(), sums_shape, vectors()]
        out += [shape(SUMS, n)] if last else list(tail)
        result = call(
            functools.partial(forward_end_kernel, column, last, heights, len(state[2])),
            tuple(out),
            "forward_end",
            4 * big,
            *operands,
            *extra,
            *krylov,
            *([u] if column == 0 else [u, z]),
        )
        if column == 0:
            krylov.append(u)
            images.append(z)
        else:
            q, z, t, *result = result
            krylov.append(q)
            images.append(z)
            totals.append(t)
        w = result[0]
        if last:
            sums = result[1]
        else:
            own, near, block = result[1:]

    def everywhere(sums):
        count = lax.axis_size("leaf")
        return lax.all_to_all(
            jnp.broadcast_to(sums[None], (count,) + sums.shape), "leaf", 0, 0
        )

    rows, square = call(
        closing_kernel,
        (shape(SUMS, n), shape(SUMS, n)),
        "closing",
        big,
        everywhere(sums),
        *krylov,
        w,
    )
    x_own, x_near, hess = call(
        answer_kernel,
        (shape(n, leaf), shape(n, leaf), shape((ITERS + 1) * ITERS, n)),
        "answer",
        big,
        everywhere(square),
        rows,
        *totals,
        *images,
    )
    x, hess = call(
        finish_kernel,
        (shape(leaf, columns), shape((ITERS + 1) * ITERS, columns)),
        "finish",
        big,
        x_own,
        from_partner(x_near, 1),
        hess,
        from_partner(hess, 1),
    )
    return (x, hess.reshape(ITERS + 1, ITERS, columns))


def solution(mesh):
    in_specs = (
        P("leaf", None),
        P("leaf", None, None),
        P("leaf", None, None),
        P("leaf", None, None),
        P(),
        P(),
        P("leaf", None, None),
        P("leaf", None, None),
        P("leaf", None, None),
        P(),
        P(),
    )
    out_specs = (P("leaf", None), P())
    return jax.shard_map(
        on_device, mesh=mesh, in_specs=in_specs, out_specs=out_specs, check_vma=False
    )
```

```python
import functools

import jax
import jax.numpy as jnp
from jax import lax
from jax.experimental import pallas as pl
from jax.experimental.pallas import tpu as pltpu
from jax.sharding import PartitionSpec as P

ITERS = 3
EPSILON = 1e-06
SUMS = 8
VMEM_LIMIT = 12 << 20
F32 = jnp.float32
BF16 = jnp.bfloat16


def from_partner(block, mask):
    count = lax.axis_size("leaf")
    return lax.ppermute(block, "leaf", [(i, i ^ mask) for i in range(count)])


def shape(*dims, dtype=F32):
    return jax.ShapeDtypeStruct(dims, dtype)


def call(kernel, out, name, flops, *args):
    local = pl.BlockSpec(memory_space=pltpu.VMEM)
    return pl.pallas_call(
        kernel,
        out_shape=out,
        in_specs=[local] * len(args),
        out_specs=jax.tree.map(lambda _: local, out),
        name=name,
        compiler_params=pltpu.CompilerParams(vmem_limit_bytes=VMEM_LIMIT),
        cost_estimate=pl.CostEstimate(flops=flops, bytes_accessed=flops // 512, transcendentals=0),
    )(*args)


def after(values, earlier):
    return lax.optimization_barrier((values, earlier))[0]


def split3(x):
    high = x.astype(BF16)
    rest = x - high.astype(F32)
    middle = rest.astype(BF16)
    low = (rest - middle.astype(F32)).astype(BF16)
    return jnp.concatenate([high, middle, low], axis=0)


def times(x, matrix, contract):
    n = x.shape[0]
    y = lax.dot_general(
        split3(x), matrix, (((1,), (contract,)), ((), ())), preferred_element_type=F32
    )
    return y[:n] + (y[n : 2 * n] + y[2 * n :])


def nn(x, matrix):
    return times(x, matrix, 0)


def nt(x, matrix):
    return times(x, matrix, 1)


def side_of(height):
    return lax.axis_index("leaf") >> height & 1


def join(c, sums, width):
    if c is None:
        n, rank = sums[0].shape[0], 0
        block = jnp.zeros((n, width), F32)
    else:
        n, rank = c.shape
        block = jnp.concatenate([c, jnp.zeros((n, width - rank), F32)], axis=1)
    lane = lax.broadcasted_iota(jnp.int32, (n, width), 1)
    for i, s in enumerate(sums):
        block = jnp.where(lane == rank + i, s, block)
    return block


def first_kernel(r_ref, columns_ref, kept_ref, sent_ref, r_kept_ref, r_sent_ref):
    rt = jnp.transpose(r_ref[...])
    half = rt.shape[0] // 2
    full = join(
        nt(rt, columns_ref[0]), [jnp.sum(rt * rt, axis=1, keepdims=True)], kept_ref.shape[1]
    )
    even = side_of(0) == 0
    kept_ref[...] = jnp.where(even, full[:half], full[half:])
    sent_ref[...] = jnp.where(even, full[half:], full[:half])
    r_kept_ref[...] = jnp.where(even, rt[:half], rt[half:])
    r_sent_ref[...] = jnp.where(even, rt[half:], rt[:half])


def meet_kernel(kept_ref, got_ref, transfer_ref, out_ref):
    rank = transfer_ref.shape[2]
    side = side_of(0)
    c = nn(kept_ref[:, :rank], transfer_ref[0, side])
    c = c + nn(got_ref[:, :rank], transfer_ref[0, 1 - side])
    sums = kept_ref[:, rank:] + got_ref[:, rank:]
    out_ref[...] = jnp.concatenate([c, sums], axis=1)


def total(own, received, rank):
    sums = [x[:, rank:] for x in [own] + received]
    if len(sums) == 2:
        return sums[0] + sums[1]
    return (sums[0] + sums[1]) + (sums[2] + sums[3])


def climb(own, received, rank, height, transfer_ref):
    side = side_of(height)
    first, second, third = received
    even = jnp.concatenate([own[:, :rank], second[:, :rank]], axis=0)
    odd = jnp.concatenate([first[:, :rank], third[:, :rank]], axis=0)
    return nn(even, transfer_ref[height, side]) + nn(odd, transfer_ref[height, 1 - side])


def middle_kernel(height, own_ref, a_ref, b_ref, ab_ref, transfer_ref, out_ref, sibling_ref):
    rank = transfer_ref.shape[2]
    own, received = own_ref[...], [a_ref[...], b_ref[...], ab_ref[...]]
    n = own.shape[0]
    both = climb(own, received, rank, height, transfer_ref)
    side = side_of(height + 1)
    c = nn(both[:n], transfer_ref[height + 1, side])
    c = c + nn(both[n:], transfer_ref[height + 1, 1 - side])
    out_ref[...] = jnp.concatenate([c, total(own, received, rank)], axis=1)
    sibling_ref[...] = both[n:]


def cross_kernel(own_ref, near_ref, *refs):
    *siblings, coupling_ref, out_ref = refs
    rank = coupling_ref.shape[2]
    side = side_of(0)
    out_ref[0] = nt(near_ref[:, :rank], coupling_ref[0, side])
    out_ref[1] = nt(own_ref[:, :rank], coupling_ref[0, 1 - side])
    for i, sibling in enumerate(siblings):
        h = i + 1
        out_ref[h + 1] = nt(sibling[:, :rank], coupling_ref[h, side_of(h)])


def block_kernel(v_ref, own_ref, near_ref, out_ref):
    out_ref[0] = nt(v_ref[0], own_ref[...])
    out_ref[1] = nt(v_ref[1], near_ref[...])


def widen_kernel(x_ref, out_ref):
    out_ref[...] = x_ref[0].astype(F32)


def narrow_kernel(x_ref, out_ref):
    out_ref[...] = x_ref[...].astype(BF16)


def swapped(matrix, earlier):
    rows, columns = matrix.shape[1:]
    matrix = after(matrix, earlier)
    wide = call(widen_kernel, shape(rows, columns), "widen", rows * columns, matrix)
    wide = from_partner(wide, 1)
    return call(narrow_kernel, shape(rows, columns, dtype=BF16), "narrow", rows * columns, wide)


def descend(heights, own, received, cross, transfer_ref, coupling_ref):
    rank = transfer_ref.shape[2]
    low = heights[0]
    side = side_of(low)
    d = nt(received[0][:, :rank], coupling_ref[low, side])
    if len(heights) == 2:
        high = heights[1]
        even, odd = received[1][:, :rank], received[2][:, :rank]
        sibling = nn(even, transfer_ref[low, side]) + nn(odd, transfer_ref[low, 1 - side])
        top = nt(sibling, coupling_ref[high, side_of(high)])
        d = d + nt(top, transfer_ref[low, side])
    for h in reversed(range(1, low)):
        d = cross[h + 1] + nt(d, transfer_ref[h, side_of(h)])
    side = side_of(0)
    d_own = cross[0] + nt(d, transfer_ref[0, side])
    d_near = cross[1] + nt(d, transfer_ref[0, 1 - side])
    return d_own, d_near


def spread(refs, heights, d_refs):
    own, received, cross, blocks, rows_own, rows_near, transfer_ref, coupling_ref = refs
    d_own, d_near = descend(heights, own, received, cross, transfer_ref, coupling_ref)
    return blocks[0] + nn(d_own, rows_own), blocks[1] + nn(d_near, rows_near)


def column_sum(x, y):
    return jnp.sum(x[0] * y[0], axis=1, keepdims=True) + jnp.sum(
        x[1] * y[1], axis=1, keepdims=True
    )


def send_off(v, sums, columns_own, columns_near, transfer_ref, own_ref, near_ref, out_ref):
    rank = transfer_ref.shape[2]
    width = out_ref.shape[1]
    c_own, c_near = nt(v[0], columns_own), nt(v[1], columns_near)
    side = side_of(0)
    c = nn(c_own, transfer_ref[0, side]) + nn(c_near, transfer_ref[0, 1 - side])
    own_ref[...] = c_own
    near_ref[...] = c_near
    out_ref[...] = join(c, sums, width)


def read(refs, received_count):
    own = refs[0][...]
    received = [r[...] for r in refs[1 : 1 + received_count]]
    cross, blocks, rows_own, rows_near, transfer, coupling = refs[
        1 + received_count : 7 + received_count
    ]
    rank = transfer.shape[2]
    values = (own, received, cross, blocks, rows_own[0], rows_near[...], transfer, coupling)
    return values, total(own, received, rank), refs[7 + received_count :]


def inverse_end_kernel(column, heights, count, *refs):
    values, totals, rest = read(refs, count)
    columns_own, columns_near, transfer_next, *rest = rest
    w = rest[0]
    krylov = rest[1 : 1 + column]
    images = rest[1 + column : 1 + 2 * column]
    u_ref, z_ref, totals_ref, own_ref, near_ref, out_ref = rest[1 + 2 * column :]
    raw = spread(values, heights, None)
    totals_ref[...] = totals
    u, z = [w[0], w[1]], list(raw)
    if column == 0:
        norm = jnp.sqrt(totals[:, 0:1] + EPSILON)
        u = [x / norm for x in u]
        z = [x / norm for x in z]
        sums = []
    else:
        for i in range(column):
            h = totals[:, i : i + 1]
            for side in range(2):
                u[side] = u[side] - h * krylov[i][side]
                z[side] = z[side] - h * images[i][side]
        sums = [column_sum(u, u)]
    for side in range(2):
        u_ref[side] = u[side]
        z_ref[side] = z[side]
    send_off(z, sums, columns_own[0], columns_near[...], transfer_next, own_ref, near_ref, out_ref)


def forward_end_kernel(column, last, heights, count, *refs):
    values, totals, rest = read(refs, count)
    if not last:
        columns_own, columns_near, transfer_next, *rest = rest
    raw = spread(values, heights, None)
    w = list(raw)
    earlier = rest[:column]
    rest = rest[column:]
    if column == 0:
        u_ref, *rest = rest
        q = [u_ref[0], u_ref[1]]
    else:
        u_ref, z_ref, q_ref, z_out_ref, totals_ref, *rest = rest
        totals_ref[...] = totals
        norm = jnp.sqrt(totals[:, 0:1] + EPSILON)
        q = [u_ref[side] / norm for side in range(2)]
        w = [x / norm for x in w]
        for side in range(2):
            q_ref[side] = q[side]
            z_out_ref[side] = z_ref[side] / norm
    sums = [column_sum(x, w) for x in list(earlier) + [q]]
    w_ref, *rest = rest
    for side in range(2):
        w_ref[side] = w[side]
    if last:
        rows = last_rows(list(earlier) + [q], w, sums)
        rest[0][...] = jnp.broadcast_to(rows[None], rest[0].shape)
    else:
        own_ref, near_ref, out_ref = rest
        send_off(
            w, sums, columns_own[0], columns_near[...], transfer_next, own_ref, near_ref, out_ref
        )


def local_projection(gram, products):
    count = len(products)
    lower, pivots, rhs = {}, [], list(products)
    for j in range(count):
        pivot = gram[j, j]
        for k in range(j):
            pivot = pivot - lower[j, k] * lower[j, k] * pivots[k][0]
        safe = pivot > 1e-6 * gram[j, j]
        inverse = jnp.where(safe, 1.0 / jnp.where(safe, pivot, 1.0), 0.0)
        pivots.append((pivot, inverse))
        for i in range(j + 1, count):
            value = gram[i, j]
            for k in range(j):
                value = value - lower[i, k] * lower[j, k] * pivots[k][0]
            lower[i, j] = value * inverse
    for j in range(count):
        for k in range(j):
            rhs[j] = rhs[j] - lower[j, k] * rhs[k]
    solved = [rhs[j] * pivots[j][1] for j in range(count)]
    for j in reversed(range(count)):
        for k in range(j + 1, count):
            solved[j] = solved[j] - lower[k, j] * solved[k]
    return solved


def last_rows(basis, w, products):
    count = len(basis)
    gram = {}
    for i in range(count):
        for k in range(i + 1):
            gram[i, k] = gram[k, i] = column_sum(basis[i], basis[k])
    p = local_projection(gram, products)
    t = list(w)
    for i, q in enumerate(basis):
        for side in range(2):
            t[side] = t[side] - p[i] * q[side]
    values = products + p + [column_sum(t, q) for q in basis] + [column_sum(t, t)]
    values += [gram[i, k] for i in range(count) for k in range(i + 1)]
    rows = jnp.transpose(join(None, values, 128))
    return jnp.concatenate([rows[:SUMS], rows[SUMS : 2 * SUMS]], axis=1)


def tree_sum(parts):
    while len(parts) > 1:
        parts = [
            parts[i] + parts[i + 1] if i + 1 < len(parts) else parts[i]
            for i in range(0, len(parts), 2)
        ]
    return parts[0]


def last_sums(got_ref):
    count = ITERS
    even = side_of(0) == 0
    half = got_ref.shape[2] // 2
    parts = []
    for chip in range(got_ref.shape[0] // 2):
        block = jnp.where(even, got_ref[2 * chip], got_ref[2 * chip + 1])
        parts.append(jnp.concatenate([block[:, :half], block[:, half:]], axis=0))
    h = tree_sum([part[:count] for part in parts])
    squares = []
    for part in parts:
        e = h - part[count : 2 * count]
        cross = part[2 * count : 3 * count]
        square = part[3 * count : 3 * count + 1]
        at = 3 * count + 1
        for i in range(count):
            square = square - 2.0 * e[i : i + 1] * cross[i : i + 1]
            for k in range(i + 1):
                factor = 1.0 if i == k else 2.0
                square = square + factor * e[i : i + 1] * e[k : k + 1] * part[at : at + 1]
                at += 1
        squares.append(square)
    return h, jnp.maximum(tree_sum(squares), 0.0)


def columns_of(rows):
    n = rows.shape[1]
    padded = jnp.concatenate([rows, jnp.zeros((128 - rows.shape[0], n), F32)], axis=0)
    return jnp.transpose(padded)


def least_squares(entries, beta_first):
    unknowns = len(entries[0])
    matrix = [list(line) for line in entries]
    target = [beta_first] + [jnp.zeros_like(beta_first) for column in range(unknowns)]
    for column in range(unknowns):
        upper_entry = matrix[column][column]
        lower_entry = matrix[column + 1][column]
        radius = jnp.sqrt(upper_entry * upper_entry + lower_entry * lower_entry)
        cosine = upper_entry / radius
        sine_value = lower_entry / radius
        for following in range(column, unknowns):
            top_value = matrix[column][following]
            bottom_value = matrix[column + 1][following]
            matrix[column][following] = cosine * top_value + sine_value * bottom_value
            matrix[column + 1][following] = cosine * bottom_value - sine_value * top_value
        top_value = target[column]
        bottom_value = target[column + 1]
        target[column] = cosine * top_value + sine_value * bottom_value
        target[column + 1] = cosine * bottom_value - sine_value * top_value
    coefficients = [None] * unknowns
    for current_row in reversed(range(unknowns)):
        remainder = target[current_row]
        for following in range(current_row + 1, unknowns):
            remainder = remainder - matrix[current_row][following] * coefficients[following]
        coefficients[current_row] = remainder / matrix[current_row][current_row]
    return coefficients


def answer_kernel(got_ref, *refs):
    totals, (z0, z1, z2, x_own_ref, x_near_ref, hess_ref) = refs[:5], refs[5:]
    width = totals[0].shape[1]

    def rows_of(ref):
        block = ref[...]
        if width < 128:
            block = jnp.concatenate([block, jnp.zeros((block.shape[0], 128 - width), F32)], 1)
        return jnp.transpose(block)

    beta_row, h0, n0, h1, n1 = [rows_of(t) for t in totals]
    rows, square = last_sums(got_ref)

    def root(x):
        return jnp.sqrt(x[0:1] + EPSILON)

    beta = root(beta_row)
    zero = jnp.zeros_like(beta)
    entries = [
        [h0[0:1], h1[0:1], rows[0:1]],
        [root(n0), h1[1:2], rows[1:2]],
        [zero, root(n1), rows[2:3]],
        [zero, zero, root(square)],
    ]
    y = least_squares(entries, beta)
    y = columns_of(jnp.concatenate(y, axis=0))
    for side, out in enumerate([x_own_ref, x_near_ref]):
        out[...] = (
            y[:, 0:1] * z0[side] + y[:, 1:2] * z1[side] + y[:, 2:3] * z2[side]
        )
    hess_ref[...] = jnp.concatenate([e for line in entries for e in line], axis=0)


def finish_kernel(x_ref, got_ref, hess_ref, hess_got_ref, out_ref, hess_out_ref):
    even = side_of(0) == 0
    own, got = x_ref[...], got_ref[...]
    out_ref[...] = jnp.transpose(
        jnp.concatenate([jnp.where(even, own, got), jnp.where(even, got, own)], axis=0)
    )
    own, got = hess_ref[...], hess_got_ref[...]
    hess = jnp.concatenate([jnp.where(even, own, got), jnp.where(even, got, own)], axis=1)
    lines, entries = hess_out_ref.shape[:2]
    for i in range(lines):
        hess_out_ref[i] = hess[i * entries : (i + 1) * entries]


class Operator:
    def __init__(self, blocks, rows, columns, transfer, coupling):
        self.blocks, self.rows, self.columns = blocks, rows, columns
        self.transfer, self.coupling = transfer, coupling
        self.near = {}

    def fetch(self, name, earlier=None):
        if name not in self.near:
            self.near[name] = swapped(getattr(self, name), earlier)
        return getattr(self, name), self.near[name]


def exchange(block, height, levels):
    masks = [1 << height]
    if height + 1 < levels:
        masks += [2 << height, 3 << height]
    return [from_partner(block, mask) for mask in masks]


def stack_kernel(own_ref, near_ref, out_ref):
    out_ref[0] = own_ref[...]
    out_ref[1] = near_ref[...]


def rounds(op, block, own, near, beside):
    levels, _, rank, _ = op.transfer.shape
    n, width = block.shape
    siblings = []
    h = 1
    unit = 6 * n * rank * rank
    while h + 2 < levels:
        received = exchange(block, h, levels)
        if h == 1 and beside is not None:
            received, beside = lax.optimization_barrier((received, beside))
        siblings.append(received[0])
        block, sibling = call(
            functools.partial(middle_kernel, h),
            (shape(n, width), shape(n, rank)),
            "middle",
            6 * unit,
            block,
            *received,
            op.transfer,
        )
        siblings.append(sibling)
        h += 2
    heights = tuple(range(h, levels))
    received = exchange(block, h, levels)
    cross = call(
        cross_kernel,
        shape(h + 1, n, rank),
        "cross",
        (h + 1) * unit,
        own,
        near,
        *siblings,
        op.coupling,
    )
    return heights, block, received, cross, beside


def on_device(
    right_side,
    diag_blocks,
    row_bases,
    column_bases,
    transfer,
    coupling,
    inverse_blocks,
    inverse_rows,
    inverse_columns,
    inverse_transfer,
    inverse_coupling,
):
    inverse = Operator(
        inverse_blocks, inverse_rows, inverse_columns, inverse_transfer, inverse_coupling
    )
    forward = Operator(diag_blocks, row_bases, column_bases, transfer, coupling)
    leaf, columns = right_side.shape
    n = columns // 2
    rank = transfer.shape[2]
    width = -(-(rank + SUMS) // 128) * 128
    unit = 6 * n * rank * rank
    big = 6 * n * rank * leaf

    kept, sent, r_kept, r_sent = call(
        first_kernel,
        (shape(n, width), shape(n, width), shape(n, leaf), shape(n, leaf)),
        "first",
        big,
        right_side,
        inverse_columns,
    )
    got = from_partner(sent, 1)
    block = call(meet_kernel, shape(n, width), "meet", 2 * unit, kept, got, inverse_transfer)
    own, near = kept, got
    r_got = from_partner(r_sent, 1)
    w = call(stack_kernel, shape(2, n, leaf), "stack", n * leaf, r_kept, r_got)

    def product(op, v):
        e_own, e_near = op.fetch("blocks")
        out = shape(2, n, leaf)
        return call(block_kernel, out, "blocks", 12 * n * leaf * leaf, v, e_own[0], e_near)

    def finish_operands(op, state):
        heights, block, received, cross, ev = state
        p_own, p_near = op.fetch("rows")
        return heights, (block, *received, cross, ev, p_own, p_near, op.transfer, op.coupling)

    def vectors():
        return shape(2, n, leaf)

    tail = (shape(n, rank), shape(n, rank), shape(n, width))
    sums_shape = shape(n, width - rank)
    krylov, images, totals = [], [], []
    for column in range(ITERS):
        last = column + 1 == ITERS
        if column == 0:
            inverse.fetch("rows", block)
            inverse.fetch("blocks", block)
            forward.fetch("columns", block)
            state = rounds(inverse, block, own, near, None)
            state = state[:4] + (product(inverse, w),)
            forward.fetch("blocks", state[1])
        else:
            state = rounds(inverse, block, own, near, product(inverse, w))
        heights, operands = finish_operands(inverse, state)
        u, z, t, own, near, block = call(
            functools.partial(inverse_end_kernel, column, heights, len(state[2])),
            (vectors(), vectors(), sums_shape) + tail,
            "inverse_end",
            4 * big,
            *operands,
            *forward.fetch("columns"),
            forward.transfer,
            w,
            *krylov,
            *images,
        )
        totals.append(t)
        if column == 0:
            forward.fetch("rows", block)
            inverse.fetch("columns", block)
        state = rounds(forward, block, own, near, product(forward, z))
        heights, operands = finish_operands(forward, state)
        extra = [] if last else [*inverse.fetch("columns"), inverse.transfer]
        out = [vectors()] if column == 0 else [vectors(), vectors(), sums_shape, vectors()]
        out += [shape(lax.axis_size("leaf"), SUMS, 2 * n)] if last else list(tail)
        result = call(
            functools.partial(forward_end_kernel, column, last, heights, len(state[2])),
            tuple(out),
            "forward_end",
            4 * big,
            *operands,
            *extra,
            *krylov,
            *([u] if column == 0 else [u, z]),
        )
        if column == 0:
            krylov.append(u)
            images.append(z)
        else:
            q, z, t, *result = result
            krylov.append(q)
            images.append(z)
            totals.append(t)
        w = result[0]
        if last:
            sums = result[1]
        else:
            own, near, block = result[1:]

    got = lax.all_to_all(sums, "leaf", 0, 0)
    x_own, x_near, hess = call(
        answer_kernel,
        (shape(n, leaf), shape(n, leaf), shape((ITERS + 1) * ITERS, n)),
        "answer",
        big,
        got,
        *totals,
        *images,
    )
    x, hess = call(
        finish_kernel,
        (shape(leaf, columns), shape(ITERS + 1, ITERS, columns)),
        "finish",
        big,
        x_own,
        from_partner(x_near, 1),
        hess,
        from_partner(hess, 1),
    )
    return (x, hess)


def solution(mesh):
    in_specs = (
        P("leaf", None),
        P("leaf", None, None),
        P("leaf", None, None),
        P("leaf", None, None),
        P(),
        P(),
        P("leaf", None, None),
        P("leaf", None, None),
        P("leaf", None, None),
        P(),
        P(),
    )
    out_specs = (P("leaf", None), P())
    return jax.shard_map(
        on_device, mesh=mesh, in_specs=in_specs, out_specs=out_specs, check_vma=False
    )
```

```python
import functools

import jax
import jax.numpy as jnp
from jax import lax
from jax.experimental import pallas as pl
from jax.experimental.pallas import tpu as pltpu
from jax.sharding import PartitionSpec as P

ITERS = 3
EPSILON = 1e-06
SUMS = 8
VMEM_LIMIT = 12 << 20
F32 = jnp.float32
BF16 = jnp.bfloat16


def from_partner(block, mask):
    count = lax.axis_size("leaf")
    return lax.ppermute(block, "leaf", [(i, i ^ mask) for i in range(count)])


def shape(*dims, dtype=F32):
    return jax.ShapeDtypeStruct(dims, dtype)


def call(kernel, out, flops, *args):
    local = pl.BlockSpec(memory_space=pltpu.VMEM)
    return pl.pallas_call(
        kernel,
        out_shape=out,
        in_specs=[local] * len(args),
        out_specs=jax.tree.map(lambda _: local, out),
        compiler_params=pltpu.CompilerParams(vmem_limit_bytes=VMEM_LIMIT),
        cost_estimate=pl.CostEstimate(flops=flops, bytes_accessed=flops // 512, transcendentals=0),
    )(*args)


def after(values, earlier):
    return lax.optimization_barrier((values, earlier))[0]


def split3(x):
    high = x.astype(BF16)
    rest = x - high.astype(F32)
    middle = rest.astype(BF16)
    low = (rest - middle.astype(F32)).astype(BF16)
    return jnp.concatenate([high, middle, low], axis=0)


def times(x, matrix, contract):
    n = x.shape[0]
    y = lax.dot_general(
        split3(x), matrix, (((1,), (contract,)), ((), ())), preferred_element_type=F32
    )
    return y[:n] + (y[n : 2 * n] + y[2 * n :])


def nn(x, matrix):
    return times(x, matrix, 0)


def nt(x, matrix):
    return times(x, matrix, 1)


def side_of(height):
    return lax.axis_index("leaf") >> height & 1


def join(c, sums, width):
    if c is None:
        n, rank = sums[0].shape[0], 0
        block = jnp.zeros((n, width), F32)
    else:
        n, rank = c.shape
        block = jnp.concatenate([c, jnp.zeros((n, width - rank), F32)], axis=1)
    lane = lax.broadcasted_iota(jnp.int32, (n, width), 1)
    for i, s in enumerate(sums):
        block = jnp.where(lane == rank + i, s, block)
    return block


def chunks(width):
    full = width // 128 * 128
    sizes, bit = [], 64
    while bit >= 1:
        if (width - full) & bit:
            sizes.append(bit)
        bit //= 2
    return full, sizes


def packed_rows(n, width):
    return n * width // 128


def pack(block):
    n, width = block.shape
    full, sizes = chunks(width)
    parts = [block[:, at : at + 128] for at in range(0, full, 128)]
    at = full
    for size in sizes:
        rows = n * size // 128
        piece = block[:, at : at + size]
        parts.append(
            jnp.concatenate([piece[i : i + rows] for i in range(0, n, rows)], axis=1)
        )
        at += size
    return jnp.concatenate(parts, axis=0)


def unpack(packed, width):
    n = packed.shape[0] * 128 // width
    full, sizes = chunks(width)
    parts, at = [], 0
    for _ in range(0, full, 128):
        parts.append(packed[at : at + n])
        at += n
    for size in sizes:
        rows = n * size // 128
        piece = packed[at : at + rows]
        parts.append(
            jnp.concatenate([piece[:, i : i + size] for i in range(0, 128, size)], axis=0)
        )
        at += rows
    return jnp.concatenate(parts, axis=1)


def first_kernel(
    r_ref, columns_ref, transfer_ref, kept_ref, sent_ref, r_kept_ref, r_sent_ref, up_ref,
    r_local, columns_local, done
):
    side = side_of(0)
    copies = [
        pltpu.make_async_copy(r_ref, r_local, done.at[0]),
        pltpu.make_async_copy(columns_ref.at[0], columns_local, done.at[1]),
        pltpu.make_async_copy(transfer_ref.at[0, side], up_ref.at[0], done.at[2]),
        pltpu.make_async_copy(transfer_ref.at[0, 1 - side], up_ref.at[1], done.at[3]),
    ]
    for copy in copies:
        copy.start()
    copies[0].wait()
    rt = jnp.transpose(r_local[...])
    half = rt.shape[0] // 2
    even = side == 0
    r_kept_ref[...] = jnp.where(even, rt[:half], rt[half:])
    r_sent_ref[...] = jnp.where(even, rt[half:], rt[:half])
    squares = jnp.sum(rt * rt, axis=1, keepdims=True)
    copies[1].wait()
    full = join(nt(rt, columns_local[...]), [squares], kept_ref.shape[1])
    kept_ref[...] = jnp.where(even, full[:half], full[half:])
    sent_ref[...] = jnp.where(even, full[half:], full[:half])
    copies[2].wait()
    copies[3].wait()


def meet_kernel(kept_ref, got_ref, up_ref, out_ref):
    rank = up_ref.shape[2]
    c = nn(kept_ref[:, :rank], up_ref[0]) + nn(got_ref[:, :rank], up_ref[1])
    sums = kept_ref[:, rank : rank + SUMS] + got_ref[:, rank : rank + SUMS]
    out_ref[...] = pack(jnp.concatenate([c, sums], axis=1))


def total(own, received, rank):
    sums = [x[:, rank:] for x in [own] + received]
    if len(sums) == 2:
        return sums[0] + sums[1]
    return (sums[0] + sums[1]) + (sums[2] + sums[3])


def climb(own, received, rank, height, transfer_ref):
    side = side_of(height)
    first, second, third = received
    even = jnp.concatenate([own[:, :rank], second[:, :rank]], axis=0)
    odd = jnp.concatenate([first[:, :rank], third[:, :rank]], axis=0)
    return nn(even, transfer_ref[height, side]) + nn(odd, transfer_ref[height, 1 - side])


def middle_kernel(height, own_ref, a_ref, b_ref, ab_ref, transfer_ref, out_ref, sibling_ref):
    rank = transfer_ref.shape[2]
    width = rank + SUMS
    own, *received = [unpack(x[...], width) for x in (own_ref, a_ref, b_ref, ab_ref)]
    n = own.shape[0]
    both = climb(own, received, rank, height, transfer_ref)
    side = side_of(height + 1)
    c = nn(both[:n], transfer_ref[height + 1, side])
    c = c + nn(both[n:], transfer_ref[height + 1, 1 - side])
    out_ref[...] = pack(jnp.concatenate([c, total(own, received, rank)], axis=1))
    sibling_ref[0] = received[0][:, :rank]
    sibling_ref[1] = both[n:]


def cross_kernel(own_ref, near_ref, *refs):
    *siblings, transfer_ref, coupling_ref, out_ref = refs
    rank = coupling_ref.shape[2]
    side = side_of(0)
    out_ref[0] = nt(near_ref[:, :rank], coupling_ref[0, side])
    out_ref[1] = nt(own_ref[:, :rank], coupling_ref[0, 1 - side])
    d = None
    for h in reversed(range(1, 2 * len(siblings) + 1)):
        term = nt(siblings[(h - 1) // 2][(h - 1) % 2], coupling_ref[h, side_of(h)])
        d = term if d is None else term + nt(d, transfer_ref[h, side_of(h)])
    out_ref[2] = jnp.zeros(out_ref.shape[1:], F32) if d is None else d


def half_block_kernel(kept_ref, sent_ref, own_ref, out_kept_ref, out_sent_ref):
    out_kept_ref[...] = nt(kept_ref[...], own_ref[0])
    out_sent_ref[...] = nt(sent_ref[...], own_ref[0])


def block_kernel(v_ref, own_ref, near_ref, out_ref):
    out_ref[0] = nt(v_ref[0], own_ref[...])
    out_ref[1] = nt(v_ref[1], near_ref[...])


def widen_kernel(x_ref, out_ref):
    out_ref[...] = x_ref[0].astype(F32)


def narrow_kernel(x_ref, out_ref):
    out_ref[...] = x_ref[...].astype(BF16)


def swapped(matrix, earlier):
    rows, columns = matrix.shape[1:]
    matrix = after(matrix, earlier)
    wide = call(widen_kernel, shape(rows, columns), rows * columns, matrix)
    wide = from_partner(wide, 1)
    return call(narrow_kernel, shape(rows, columns, dtype=BF16), rows * columns, wide)


def composite_kernel(heights, transfer_ref, coupling_ref, out_ref):
    rank = transfer_ref.shape[2]
    low = heights[0]
    side = side_of(low)
    row = lax.broadcasted_iota(jnp.int32, (rank, rank), 0)
    lane = lax.broadcasted_iota(jnp.int32, (rank, rank), 1)
    m = nt(jnp.where(row == lane, 1.0, 0.0).astype(F32), coupling_ref[low, side])
    if len(heights) == 2:
        high = heights[1]
        rest = jnp.concatenate(
            [transfer_ref[low, side].astype(F32), transfer_ref[low, 1 - side].astype(F32)], axis=0
        )
        rest = nt(rest, coupling_ref[high, side_of(high)])
        m = jnp.concatenate([m, nt(rest, transfer_ref[low, side])], axis=0)
    for h in reversed(range(1, low)):
        m = nt(m, transfer_ref[h, side_of(h)])
    size = m.shape[0]
    terms = split3(m)
    for i in range(3):
        out_ref[i] = terms[i * size : (i + 1) * size]


def through(x, composite_ref, at):
    n, rank = x.shape
    terms = split3(x)
    result = None
    for i in reversed(range(3)):
        matrix = composite_ref[i, at : at + rank]
        y = jnp.dot(terms[: (3 - i) * n], matrix, preferred_element_type=F32)
        for k in reversed(range(3 - i)):
            part = y[k * n : (k + 1) * n]
            result = part if result is None else result + part
    return result


def descend(heights, received, cross, transfer_ref, coupling_ref, composite_ref):
    rank = transfer_ref.shape[2]
    low = heights[0]
    if composite_ref is not None:
        d = None
        blocks = received if len(heights) == 2 else received[:1]
        for i, block in enumerate(blocks):
            part = through(block[:, :rank], composite_ref, i * rank)
            d = part if d is None else d + part
    else:
        side = side_of(low)
        d = nt(received[0][:, :rank], coupling_ref[low, side])
        if len(heights) == 2:
            high = heights[1]
            even, odd = received[1][:, :rank], received[2][:, :rank]
            sibling = nn(even, transfer_ref[low, side]) + nn(odd, transfer_ref[low, 1 - side])
            top = nt(sibling, coupling_ref[high, side_of(high)])
            d = d + nt(top, transfer_ref[low, side])
        for h in reversed(range(1, low)):
            d = nt(d, transfer_ref[h, side_of(h)])
    d = cross[2] + d
    side = side_of(0)
    d_own = cross[0] + nt(d, transfer_ref[0, side])
    d_near = cross[1] + nt(d, transfer_ref[0, 1 - side])
    return d_own, d_near


def spread(values, heights):
    received, cross, blocks, rows_own, rows_near, transfer, coupling, composite = values
    d_own, d_near = descend(heights, received, cross, transfer, coupling, composite)
    return blocks[0] + nn(d_own, rows_own), blocks[1] + nn(d_near, rows_near)


def column_sum(x, y):
    return jnp.sum(x[0] * y[0] + x[1] * y[1], axis=1, keepdims=True)


def send_off(v, sums, columns_own, columns_near, transfer_ref, own_ref, near_ref, out_ref):
    rank = transfer_ref.shape[2]
    width = rank + SUMS
    c_own, c_near = nt(v[0], columns_own), nt(v[1], columns_near)
    side = side_of(0)
    c = nn(c_own, transfer_ref[0, side]) + nn(c_near, transfer_ref[0, 1 - side])
    own_ref[...] = c_own
    near_ref[...] = c_near
    out_ref[...] = pack(join(c, sums, width))


def read(refs, received_count, composed):
    cross, blocks, rows_own, rows_near, transfer, coupling = refs[
        1 + received_count : 7 + received_count
    ]
    rest = refs[7 + received_count :]
    composite = None
    if composed:
        composite, *rest = rest
    rank = transfer.shape[2]
    own, *received = [unpack(r[...], rank + SUMS) for r in refs[: 1 + received_count]]
    values = (
        received, cross, blocks, rows_own[0], rows_near[...], transfer, coupling, composite
    )
    return values, total(own, received, rank), rest


def inverse_end_kernel(column, heights, count, composed, *refs):
    values, totals, rest = read(refs, count, composed)
    columns_own, columns_near, transfer_next, *rest = rest
    w = rest[0]
    krylov = rest[1 : 1 + column]
    images = rest[1 + column : 1 + 2 * column]
    u_ref, z_ref, totals_ref, own_ref, near_ref, out_ref, *given = rest[1 + 2 * column :]
    raw = spread(values, heights)
    totals_ref[...] = totals
    u, z = [w[0], w[1]], list(raw)
    if column == 0:
        norm = jnp.sqrt(totals[:, 0:1] + EPSILON)
        u = [x / norm for x in u]
        z = [x / norm for x in z]
        sums = []
    else:
        for i in range(column):
            h = totals[:, i : i + 1]
            for side in range(2):
                u[side] = u[side] - h * krylov[i][side]
                z[side] = z[side] - h * images[i][side]
        sums = [column_sum(u, u)]
    for side in range(2):
        u_ref[side] = u[side]
        z_ref[side] = z[side]
    if column == 0:
        given[0][...] = z[1]
    send_off(z, sums, columns_own[0], columns_near[...], transfer_next, own_ref, near_ref, out_ref)


def gram_kernel(*refs):
    *basis, out_ref = refs
    count = len(basis)
    gram, lower, pivots, inverses = {}, {}, [], []
    for i, x in enumerate(basis):
        for k, y in enumerate(basis[: i + 1]):
            gram[i, k] = column_sum(x, y)
    for j in range(count):
        pivot = gram[j, j]
        for k in range(j):
            pivot = pivot - lower[j, k] * lower[j, k] * pivots[k]
        safe = pivot > 1e-6 * gram[j, j]
        inverse = jnp.where(safe, 1.0 / jnp.where(safe, pivot, 1.0), 0.0)
        pivots.append(pivot)
        inverses.append(inverse)
        for i in range(j + 1, count):
            value = gram[i, j]
            for k in range(j):
                value = value - lower[i, k] * lower[j, k] * pivots[k]
            lower[i, j] = value * inverse
    values = [gram[i, k] for i in range(count) for k in range(i + 1)]
    values += [lower[i, k] for i in range(count) for k in range(i)] + inverses
    for i, value in enumerate(values):
        out_ref[i] = jnp.broadcast_to(value, out_ref.shape[1:])


def forward_end_kernel(column, last, heights, count, composed, *refs):
    values, totals, rest = read(refs, count, composed)
    if last:
        gram_ref, *rest = rest
        known, rest = rest[: 2 * column], rest[2 * column :]
    else:
        columns_own, columns_near, transfer_next, *rest = rest
    w = list(spread(values, heights))
    earlier = rest[:column]
    rest = rest[column:]
    norm = None
    if column == 0:
        u_ref, *rest = rest
        q = [u_ref[0], u_ref[1]]
    else:
        u_ref, z_ref, q_ref, z_out_ref, z_given_ref, totals_ref, *rest = rest
        totals_ref[...] = totals
        norm = jnp.sqrt(totals[:, 0:1] + EPSILON)
        q = [u_ref[side] / norm for side in range(2)]
        w = [x / norm for x in w]
        for side in range(2):
            q_ref[side] = q[side]
            z = z_ref[side] / norm
            z_out_ref[side] = z
        z_given_ref[...] = z
    sums = [column_sum(x, w) for x in list(earlier) + [q]]
    if last:
        rows_ref, known_ref = rest
        rows = last_rows(list(earlier) + [q], w, sums, gram_ref, norm)
        rows_ref[...] = jnp.broadcast_to(rows[None], rows_ref.shape)
        values = []
        for i in range(2 * column):
            values += [known[i][:, k : k + 1] for k in range((i + 1) // 2 if i % 2 else 1)]
        values.append(totals[:, 0:1])
        known_ref[...] = jnp.transpose(join(None, values, 128))[:SUMS]
    else:
        w_ref, own_ref, near_ref, out_ref = rest
        for side in range(2):
            w_ref[side] = w[side]
        send_off(
            w, sums, columns_own[0], columns_near[...], transfer_next, own_ref, near_ref, out_ref
        )


def local_projection(lower, inverses, products):
    count = len(products)
    rhs = list(products)
    for j in range(count):
        for k in range(j):
            rhs[j] = rhs[j] - lower[j, k] * rhs[k]
    solved = [rhs[j] * inverses[j] for j in range(count)]
    for j in reversed(range(count)):
        for k in range(j + 1, count):
            solved[j] = solved[j] - lower[k, j] * solved[k]
    return solved


def last_rows(basis, w, products, gram_ref, norm):
    count = len(basis)
    n, leaf = w[0].shape

    def wide(x):
        return jnp.broadcast_to(x, (n, 128))

    norm = wide(norm)
    products = [wide(x) for x in products]
    gram, at = [], 0
    for i in range(count):
        for k in range(i + 1):
            value = gram_ref[at]
            if i + 1 == count:
                value = value / norm
            if k + 1 == count:
                value = value / norm
            gram.append(value)
            at += 1
    lower = {}
    for i in range(count):
        for k in range(i):
            lower[i, k] = gram_ref[at]
            at += 1
    inverses = [gram_ref[at + i] for i in range(count)]
    p = local_projection(lower, inverses, products[:-1] + [products[-1] * norm])
    p[-1] = p[-1] * norm
    t = list(w)
    for i, q in enumerate(basis):
        factor = jnp.concatenate([p[i]] * (leaf // 128), axis=1)
        for side in range(2):
            t[side] = t[side] - factor * q[side]
    values = products + p + [column_sum(t, q) for q in basis] + [column_sum(t, t)] + gram
    rows = jnp.transpose(join(None, values, 128))
    return jnp.concatenate([rows[:SUMS], rows[SUMS : 2 * SUMS]], axis=1)


def tree_sum(parts):
    while len(parts) > 1:
        parts = [
            parts[i] + parts[i + 1] if i + 1 < len(parts) else parts[i]
            for i in range(0, len(parts), 2)
        ]
    return parts[0]


def last_sums(got_ref):
    count = ITERS
    half = got_ref.shape[2] // 2
    parts = []
    for chip in range(got_ref.shape[0] // 2):
        low, high = got_ref[2 * chip], got_ref[2 * chip + 1]
        upper = jnp.concatenate([low[:, :half], high[:, :half]], axis=1)
        lower = jnp.concatenate([low[:, half:], high[:, half:]], axis=1)
        parts.append(jnp.concatenate([upper, lower], axis=0))
    h = tree_sum([part[:count] for part in parts])
    squares = []
    for part in parts:
        e = h - part[count : 2 * count]
        square = part[3 * count : 3 * count + 1]
        at = 3 * count + 1
        for i in range(count):
            row = e[i : i + 1]
            square = square - 2.0 * row * part[2 * count + i : 2 * count + i + 1]
            for k in range(i + 1):
                factor = 1.0 if i == k else 2.0
                square = square + factor * row * e[k : k + 1] * part[at : at + 1]
                at += 1
        squares.append(square)
    return h, jnp.maximum(tree_sum(squares), 0.0)


def columns_of(rows):
    n = rows.shape[1]
    padded = jnp.concatenate([rows, jnp.zeros((128 - rows.shape[0], n), F32)], axis=0)
    return jnp.transpose(padded)


def least_squares(entries, beta_first):
    unknowns = len(entries[0])
    matrix = [list(line) for line in entries]
    target = [beta_first] + [jnp.zeros_like(beta_first) for _ in range(unknowns)]
    for column in range(unknowns):
        upper_entry = matrix[column][column]
        lower_entry = matrix[column + 1][column]
        radius = jnp.sqrt(upper_entry * upper_entry + lower_entry * lower_entry)
        cosine = upper_entry / radius
        sine_value = lower_entry / radius
        for following in range(column, unknowns):
            top_value = matrix[column][following]
            bottom_value = matrix[column + 1][following]
            matrix[column][following] = cosine * top_value + sine_value * bottom_value
            matrix[column + 1][following] = cosine * bottom_value - sine_value * top_value
        top_value = target[column]
        bottom_value = target[column + 1]
        target[column] = cosine * top_value + sine_value * bottom_value
        target[column + 1] = cosine * bottom_value - sine_value * top_value
    coefficients = [None] * unknowns
    for current_row in reversed(range(unknowns)):
        remainder = target[current_row]
        for following in range(current_row + 1, unknowns):
            remainder = remainder - matrix[current_row][following] * coefficients[following]
        coefficients[current_row] = remainder / matrix[current_row][current_row]
    return coefficients


def answer_kernel(got_ref, mine_ref, other_ref, *refs):
    given = refs[:ITERS]
    images = refs[ITERS : 2 * ITERS]
    out_ref, hess_ref = refs[2 * ITERS :]
    even = side_of(0) == 0

    def ordered(own, got, axis):
        return jnp.concatenate(
            [jnp.where(even, own, got), jnp.where(even, got, own)], axis=axis
        )

    known = ordered(mine_ref[...], other_ref[...], 1)
    last, square = last_sums(got_ref)

    def root(x):
        return jnp.sqrt(x + EPSILON)

    row = [known[i : i + 1] for i in range(SUMS)]
    beta = root(row[0])
    zero = jnp.zeros_like(beta)
    entries = [[zero] * ITERS for _ in range(ITERS + 1)]
    at = 1
    for column in range(ITERS - 1):
        for i in range(column + 1):
            entries[i][column] = row[at]
            at += 1
        entries[column + 1][column] = root(row[at])
        at += 1
    for i in range(ITERS):
        entries[i][ITERS - 1] = last[i : i + 1]
    entries[ITERS][ITERS - 1] = root(square)
    y = columns_of(jnp.concatenate(least_squares(entries, beta), axis=0))
    x = None
    for i in range(ITERS):
        term = y[:, i : i + 1] * ordered(images[i][0], given[i][...], 0)
        x = term if x is None else x + term
    out_ref[...] = jnp.transpose(x)
    for i, line in enumerate(entries):
        hess_ref[i] = jnp.concatenate(line, axis=0)


class Operator:
    def __init__(self, tag, blocks, rows, columns, transfer, coupling):
        self.tag = tag
        self.blocks, self.rows, self.columns = blocks, rows, columns
        self.transfer, self.coupling = transfer, coupling
        self.near = {}

    def fetch(self, name, earlier=None):
        if name not in self.near:
            self.near[name] = swapped(getattr(self, name), earlier)
        return getattr(self, name), self.near[name]


def exchange(block, height, levels):
    masks = [1 << height]
    if height + 1 < levels:
        masks += [2 << height, 3 << height]
    return [from_partner(block, mask) for mask in masks]


def stack_kernel(own_ref, near_ref, out_ref):
    out_ref[0] = own_ref[...]
    out_ref[1] = near_ref[...]


def rounds(op, block, own, near, n, beside):
    levels, _, rank, _ = op.transfer.shape
    width = rank + SUMS
    siblings = []
    h = 1
    unit = 6 * n * rank * rank
    results = None
    while h + 2 < levels:
        received = exchange(block, h, levels)
        if h == 1:
            results = beside(received[0])
            received, results = lax.optimization_barrier((received, results))
        block, sibling = call(
            functools.partial(middle_kernel, h),
            (shape(packed_rows(n, width), 128), shape(2, n, rank)),
            6 * unit,
            block,
            *received,
            op.transfer,
        )
        siblings.append(sibling)
        h += 2
    heights = tuple(range(h, levels))
    received = exchange(block, h, levels)
    if results is None:
        results = beside(received[0])
    cross = call(
        cross_kernel,
        shape(3, n, rank),
        (h + 1) * unit,
        own,
        near,
        *siblings,
        op.transfer,
        op.coupling,
    )
    return heights, block, received, cross, results


def device_body(
    right_side,
    diag_blocks,
    row_bases,
    column_bases,
    transfer,
    coupling,
    inverse_blocks,
    inverse_rows,
    inverse_columns,
    inverse_transfer,
    inverse_coupling,
):
    inverse = Operator(
        "inverse", inverse_blocks, inverse_rows, inverse_columns, inverse_transfer, inverse_coupling
    )
    forward = Operator("forward", diag_blocks, row_bases, column_bases, transfer, coupling)
    leaf, columns = right_side.shape
    n = columns // 2
    rank = transfer.shape[2]
    width = -(-(rank + SUMS) // 128) * 128
    unit = 6 * n * rank * rank
    big = 6 * n * rank * leaf

    local = pl.BlockSpec(memory_space=pltpu.VMEM)
    away = pl.BlockSpec(memory_space=pltpu.HBM)
    kept, sent, r_kept, r_sent, up = pl.pallas_call(
        first_kernel,
        out_shape=(
            shape(n, width),
            shape(n, width),
            shape(n, leaf),
            shape(n, leaf),
            shape(2, rank, rank, dtype=BF16),
        ),
        in_specs=[away] * 3,
        out_specs=(local,) * 5,
        scratch_shapes=[
            pltpu.VMEM((leaf, columns), F32),
            pltpu.VMEM((rank, leaf), BF16),
            pltpu.SemaphoreType.DMA((4,)),
        ],
        name="first",
        compiler_params=pltpu.CompilerParams(vmem_limit_bytes=VMEM_LIMIT),
    )(
        *[
            pltpu.with_memory_space_constraint(x, pltpu.HBM)
            for x in (right_side, inverse_columns, inverse_transfer)
        ]
    )
    got = from_partner(sent, 1)
    block_rows = packed_rows(n, rank + SUMS)
    block = call(meet_kernel, shape(block_rows, 128), 2 * unit, kept, got, up)
    own, near = kept, got

    def product(op, v):
        e_own, e_near = op.fetch("blocks")
        out = shape(2, n, leaf)
        return call(block_kernel, out, 12 * n * leaf * leaf, v, e_own[0], e_near)

    def first_product():
        ev_kept, ev_sent = call(
            half_block_kernel,
            (shape(n, leaf), shape(n, leaf)),
            12 * n * leaf * leaf,
            r_kept,
            r_sent,
            inverse_blocks,
        )
        return ev_kept, ev_sent

    composites = {}

    def compose(op, heights, earlier):
        out = shape(3, (2 * len(heights) - 1) * rank, rank, dtype=BF16)
        composites[op.tag] = call(
            functools.partial(composite_kernel, heights),
            out,
            20 * rank**3,
            after(op.transfer, earlier),
            op.coupling,
        )

    def finish_operands(op, state, ev):
        heights, block, received, cross, _ = state
        p_own, p_near = op.fetch("rows")
        operands = (block, *received, cross, ev, p_own, p_near, op.transfer, op.coupling)
        if op.tag in composites:
            return heights, operands + (composites[op.tag],)
        return heights, operands

    def vectors():
        return shape(2, n, leaf)

    tail = (shape(n, rank), shape(n, rank), shape(block_rows, 128))
    sums_shape = shape(n, SUMS)
    krylov, images, given, totals = [], [], [], []
    for column in range(ITERS):
        last = column + 1 == ITERS
        if column == 0:

            def beside(received):
                return first_product()

            state = rounds(inverse, block, own, near, n, beside)
            ev_kept, ev_sent = state[4]
            inverse.fetch("rows", block)
            forward.fetch("columns", block)
            r_got = from_partner(r_sent, 1)
            ev_got = from_partner(ev_sent, 1)
            w = call(stack_kernel, shape(2, n, leaf), n * leaf, r_kept, r_got)
            ev = call(stack_kernel, shape(2, n, leaf), n * leaf, ev_kept, ev_got)
            forward.fetch("blocks", state[1])
        else:
            state = rounds(inverse, block, own, near, n, lambda _: product(inverse, w))
            ev = state[4]
        heights, operands = finish_operands(inverse, state, ev)
        if column == 1:
            compose(forward, heights, block)
        more = (shape(n, leaf),) if column == 0 else ()
        u, z, t, own, near, block, *z_given = call(
            functools.partial(inverse_end_kernel, column, heights, len(state[2]), column > 0),
            (vectors(), vectors(), sums_shape) + tail + more,
            4 * big,
            *operands,
            *forward.fetch("columns"),
            forward.transfer,
            w,
            *krylov,
            *images,
        )
        totals.append(t)

        def beside_forward(received):
            if column == 0:
                forward.fetch("rows", u)
                inverse.fetch("columns", u)
            return product(forward, z)

        state = rounds(forward, block, own, near, n, beside_forward)
        if column == 0:
            inverse.fetch("blocks", state[1])
        heights, operands = finish_operands(forward, state, state[4])
        if column == 0:
            compose(inverse, heights, block)
        if last:
            count = column + 1
            out = shape(count * (count + 1), n, 128)
            gram = call(gram_kernel, out, big, *krylov, u)
            extra = [gram, *totals]
        else:
            extra = [*inverse.fetch("columns"), inverse.transfer]
        out = []
        if column > 0:
            out += [vectors(), vectors(), shape(n, leaf), sums_shape]
        if last:
            out += [shape(lax.axis_size("leaf"), SUMS, 2 * n), shape(SUMS, n)]
        else:
            out += [vectors(), *tail]
        result = call(
            functools.partial(forward_end_kernel, column, last, heights, len(state[2]), column > 0),
            tuple(out),
            4 * big,
            *operands,
            *extra,
            *krylov,
            *([u] if column == 0 else [u, z]),
        )
        if column == 0:
            krylov.append(u)
            images.append(z)
            given.append(z_given[0])
        else:
            q, z, z_given, t, *result = result
            krylov.append(q)
            images.append(z)
            given.append(z_given)
            totals.append(t)
        if last:
            rows, known = result
        else:
            w, own, near, block = result

    got = lax.all_to_all(rows, "leaf", 0, 0)
    x, hess = call(
        answer_kernel,
        (shape(leaf, columns), shape(ITERS + 1, ITERS, columns)),
        big,
        got,
        known,
        from_partner(known, 1),
        *[from_partner(z, 1) for z in given],
        *images,
    )
    return (x, hess)


def solution(mesh):
    in_specs = (
        P("leaf", None),
        P("leaf", None, None),
        P("leaf", None, None),
        P("leaf", None, None),
        P(),
        P(),
        P("leaf", None, None),
        P("leaf", None, None),
        P("leaf", None, None),
        P(),
        P(),
    )
    out_specs = (P("leaf", None), P())
    return jax.shard_map(
        device_body, mesh=mesh, in_specs=in_specs, out_specs=out_specs, check_vma=False
    )
```

```python
import functools

import jax
import jax.numpy as jnp
from jax import lax
from jax.experimental import pallas as pl
from jax.experimental.pallas import tpu as pltpu
from jax.sharding import PartitionSpec as P

ITERS = 3
EPSILON = 1e-06
SUMS = 8
VMEM_LIMIT = 12 << 20
F32 = jnp.float32
BF16 = jnp.bfloat16


def from_partner(block, mask):
    count = lax.axis_size("leaf")
    return lax.ppermute(block, "leaf", [(i, i ^ mask) for i in range(count)])


def with_partner(block):
    return from_partner(block, 1)


def shape(*dims, dtype=F32):
    return jax.ShapeDtypeStruct(dims, dtype)


def call(kernel, out, flops, *args, scratch=()):
    local = pl.BlockSpec(memory_space=pltpu.VMEM)
    return pl.pallas_call(
        kernel,
        out_shape=out,
        in_specs=[local] * len(args),
        out_specs=jax.tree.map(lambda _: local, out),
        scratch_shapes=scratch,
        compiler_params=pltpu.CompilerParams(vmem_limit_bytes=VMEM_LIMIT),
        cost_estimate=pl.CostEstimate(flops=flops, bytes_accessed=flops // 512, transcendentals=0),
    )(*args)


def after(values, earlier):
    return lax.optimization_barrier((values, earlier))[0]


def split3(x):
    high = x.astype(BF16)
    rest = x - high.astype(F32)
    middle = rest.astype(BF16)
    low = (rest - middle.astype(F32)).astype(BF16)
    return jnp.concatenate([high, middle, low], axis=0)


def times(x, matrix, contract):
    n = x.shape[0]
    y = lax.dot_general(
        split3(x), matrix, (((1,), (contract,)), ((), ())), preferred_element_type=F32
    )
    return y[:n] + (y[n : 2 * n] + y[2 * n :])


def nn(x, matrix):
    return times(x, matrix, 0)


def nt(x, matrix):
    return times(x, matrix, 1)


def side_of(height):
    return lax.axis_index("leaf") >> height & 1


def join(c, sums, width):
    if c is None:
        n, rank = sums[0].shape[0], 0
        block = jnp.zeros((n, width), F32)
    else:
        n, rank = c.shape
        block = jnp.concatenate([c, jnp.zeros((n, width - rank), F32)], axis=1)
    lane = lax.broadcasted_iota(jnp.int32, (n, width), 1)
    for i, s in enumerate(sums):
        block = jnp.where(lane == rank + i, s, block)
    return block


def padded(block):
    n, width = block.shape
    return jnp.concatenate([block, jnp.zeros((n, -width % 128), F32)], axis=1)


def chunks(width):
    full = width // 128 * 128
    sizes, bit = [], 64
    while bit >= 1:
        if (width - full) & bit:
            sizes.append(bit)
        bit //= 2
    return full, sizes


def pack(block):
    n, width = block.shape
    full, sizes = chunks(width)
    parts = [block[:, at : at + 128] for at in range(0, full, 128)]
    at = full
    for size in sizes:
        rows = n * size // 128
        piece = block[:, at : at + size]
        parts.append(
            jnp.concatenate([piece[i : i + rows] for i in range(0, n, rows)], axis=1)
        )
        at += size
    return jnp.concatenate(parts, axis=0)


def unpack(packed, width):
    if packed.shape[1] > 128:
        return packed[:, :width]
    n = packed.shape[0] * 128 // width
    full, sizes = chunks(width)
    parts, at = [], 0
    for _ in range(0, full, 128):
        parts.append(packed[at : at + n])
        at += n
    for size in sizes:
        rows = n * size // 128
        piece = packed[at : at + rows]
        parts.append(
            jnp.concatenate([piece[:, i : i + size] for i in range(0, 128, size)], axis=0)
        )
        at += rows
    return jnp.concatenate(parts, axis=1)


def first_kernel(
    r_ref, columns_ref, transfer_ref, kept_ref, sent_ref, r_kept_ref, r_sent_ref, up_ref,
    r_local, columns_local, done
):
    side = side_of(0)
    copies = [
        pltpu.make_async_copy(r_ref, r_local, done.at[0]),
        pltpu.make_async_copy(columns_ref.at[0], columns_local, done.at[1]),
        pltpu.make_async_copy(transfer_ref.at[0, side], up_ref.at[0], done.at[2]),
        pltpu.make_async_copy(transfer_ref.at[0, 1 - side], up_ref.at[1], done.at[3]),
    ]
    for copy in copies:
        copy.start()
    copies[0].wait()
    rt = jnp.transpose(r_local[...])
    half = rt.shape[0] // 2
    even = side == 0
    r_kept_ref[...] = jnp.where(even, rt[:half], rt[half:])
    r_sent_ref[...] = jnp.where(even, rt[half:], rt[:half])
    squares = jnp.sum(rt * rt, axis=1, keepdims=True)
    copies[1].wait()
    full = join(nt(rt, columns_local[...]), [squares], kept_ref.shape[1])
    kept_ref[...] = jnp.where(even, full[:half], full[half:])
    sent_ref[...] = jnp.where(even, full[half:], full[:half])
    copies[2].wait()
    copies[3].wait()


def meet_kernel(own_ref, near_ref, up_ref, out_ref, c_ref):
    rank = up_ref.shape[2]
    c_ref[0] = own_ref[:, :rank]
    c_ref[1] = near_ref[:, :rank]
    c = nn(c_ref[0], up_ref[0]) + nn(c_ref[1], up_ref[1])
    sums = own_ref[:, rank : rank + SUMS] + near_ref[:, rank : rank + SUMS]
    out_ref[...] = padded(jnp.concatenate([c, sums], axis=1))


def total(own, received, rank):
    sums = [x[:, rank:] for x in [own] + received]
    if len(sums) == 2:
        return sums[0] + sums[1]
    return (sums[0] + sums[1]) + (sums[2] + sums[3])


def climb(own, received, rank, height, transfer_ref):
    side = side_of(height)
    first, second, third = received
    even = jnp.concatenate([own[:, :rank], second[:, :rank]], axis=0)
    odd = jnp.concatenate([first[:, :rank], third[:, :rank]], axis=0)
    return nn(even, transfer_ref[height, side]) + nn(odd, transfer_ref[height, 1 - side])


def middle_kernel(height, own_ref, a_ref, b_ref, ab_ref, transfer_ref, out_ref, sibling_ref):
    rank = transfer_ref.shape[2]
    width = rank + SUMS
    own, *received = [unpack(x[...], width) for x in (own_ref, a_ref, b_ref, ab_ref)]
    n = own.shape[0]
    both = climb(own, received, rank, height, transfer_ref)
    side = side_of(height + 1)
    c = nn(both[:n], transfer_ref[height + 1, side])
    c = c + nn(both[n:], transfer_ref[height + 1, 1 - side])
    out_ref[...] = pack(jnp.concatenate([c, total(own, received, rank)], axis=1))
    sibling_ref[0] = received[0][:, :rank]
    sibling_ref[1] = both[n:]


def cross_kernel(c_ref, *refs):
    *siblings, transfer_ref, coupling_ref, out_ref = refs
    side = side_of(0)
    out_ref[0] = nt(c_ref[1], coupling_ref[0, side])
    out_ref[1] = nt(c_ref[0], coupling_ref[0, 1 - side])
    d = None
    for h in reversed(range(1, 2 * len(siblings) + 1)):
        term = nt(siblings[(h - 1) // 2][(h - 1) % 2], coupling_ref[h, side_of(h)])
        d = term if d is None else term + nt(d, transfer_ref[h, side_of(h)])
    out_ref[2] = jnp.zeros(out_ref.shape[1:], F32) if d is None else d


def block_rows(v_ref, matrix_ref, out_ref, split_ref):
    n, leaf = v_ref.shape
    chunk = min(512, leaf)
    split_ref[...] = split3(v_ref[...])

    def step(i, carry):
        at = pl.multiple_of(i * chunk, chunk)
        y = lax.dot_general(
            split_ref[...],
            matrix_ref[pl.ds(at, chunk)],
            (((1,), (1,)), ((), ())),
            preferred_element_type=F32,
        )
        out_ref[:, pl.ds(at, chunk)] = y[:n] + (y[n : 2 * n] + y[2 * n :])
        return carry

    lax.fori_loop(0, leaf // chunk, step, 0)


def half_block_kernel(kept_ref, sent_ref, own_ref, out_kept_ref, out_sent_ref, split_ref):
    block_rows(kept_ref, own_ref.at[0], out_kept_ref, split_ref)
    block_rows(sent_ref, own_ref.at[0], out_sent_ref, split_ref)


def block_kernel(v_ref, own_ref, near_ref, out_ref, split_ref):
    block_rows(v_ref.at[0], own_ref, out_ref.at[0], split_ref)
    block_rows(v_ref.at[1], near_ref, out_ref.at[1], split_ref)


def widen_kernel(x_ref, out_ref):
    out_ref[...] = x_ref[0].astype(F32)


def narrow_kernel(x_ref, out_ref):
    out_ref[...] = x_ref[...].astype(BF16)


def swapped(matrix, earlier):
    rows, columns = matrix.shape[1:]
    matrix = after(matrix, earlier)
    wide = call(widen_kernel, shape(rows, columns), rows * columns, matrix)
    wide = with_partner(wide)
    return call(narrow_kernel, shape(rows, columns, dtype=BF16), rows * columns, wide)


def composite_kernel(heights, transfer_ref, coupling_ref, out_ref):
    rank = transfer_ref.shape[2]
    low = heights[0]
    side = side_of(low)
    row = lax.broadcasted_iota(jnp.int32, (rank, rank), 0)
    lane = lax.broadcasted_iota(jnp.int32, (rank, rank), 1)
    m = nt(jnp.where(row == lane, 1.0, 0.0).astype(F32), coupling_ref[low, side])
    if len(heights) == 2:
        high = heights[1]
        rest = jnp.concatenate(
            [transfer_ref[low, side].astype(F32), transfer_ref[low, 1 - side].astype(F32)], axis=0
        )
        rest = nt(rest, coupling_ref[high, side_of(high)])
        m = jnp.concatenate([m, nt(rest, transfer_ref[low, side])], axis=0)
    for h in reversed(range(1, low)):
        m = nt(m, transfer_ref[h, side_of(h)])
    size = m.shape[0]
    terms = split3(m)
    for i in range(3):
        out_ref[i] = terms[i * size : (i + 1) * size]


def through(x, composite_ref, at):
    n, rank = x.shape
    terms = split3(x)
    result = None
    for i in reversed(range(3)):
        matrix = composite_ref[i, at : at + rank]
        y = jnp.dot(terms[: (3 - i) * n], matrix, preferred_element_type=F32)
        for k in reversed(range(3 - i)):
            part = y[k * n : (k + 1) * n]
            result = part if result is None else result + part
    return result


def descend(heights, received, cross, transfer_ref, coupling_ref, composite_ref):
    rank = transfer_ref.shape[2]
    low = heights[0]
    if composite_ref is not None:
        d = None
        blocks = received if len(heights) == 2 else received[:1]
        for i, block in enumerate(blocks):
            part = through(block[:, :rank], composite_ref, i * rank)
            d = part if d is None else d + part
    else:
        side = side_of(low)
        d = nt(received[0][:, :rank], coupling_ref[low, side])
        if len(heights) == 2:
            high = heights[1]
            even, odd = received[1][:, :rank], received[2][:, :rank]
            sibling = nn(even, transfer_ref[low, side]) + nn(odd, transfer_ref[low, 1 - side])
            top = nt(sibling, coupling_ref[high, side_of(high)])
            d = d + nt(top, transfer_ref[low, side])
        for h in reversed(range(1, low)):
            d = nt(d, transfer_ref[h, side_of(h)])
    d = cross[2] + d
    side = side_of(0)
    d_own = cross[0] + nt(d, transfer_ref[0, side])
    d_near = cross[1] + nt(d, transfer_ref[0, 1 - side])
    return d_own, d_near


def spread(values, heights):
    received, cross, blocks, rows_own, rows_near, transfer, coupling, composite = values
    d_own, d_near = descend(heights, received, cross, transfer, coupling, composite)
    return blocks[0] + nn(d_own, rows_own), blocks[1] + nn(d_near, rows_near)


def column_sum(x, y):
    return jnp.sum(x[0] * y[0] + x[1] * y[1], axis=1, keepdims=True)


def read(refs, received_count, composed):
    cross, blocks, rows_own, rows_near, transfer, coupling = refs[
        1 + received_count : 7 + received_count
    ]
    rest = refs[7 + received_count :]
    composite = None
    if composed:
        composite, *rest = rest
    rank = transfer.shape[2]
    own, *received = [unpack(r[...], rank + SUMS) for r in refs[: 1 + received_count]]
    values = (
        received, cross, blocks, rows_own[0], rows_near[...], transfer, coupling, composite
    )
    return values, total(own, received, rank), rest


def head(refs, heights, count, composed, products_ref, link_ref):
    cross, transfer, coupling = refs[1 + count : 4 + count]
    rest = refs[4 + count :]
    composite = None
    if composed:
        composite, *rest = rest
    rank = transfer.shape[2]
    own, *received = [unpack(r[...], rank + SUMS) for r in refs[: 1 + count]]
    d = descend(heights, received, cross, transfer, coupling, composite)
    c = [products_ref[i] + through(d[i], link_ref, i * rank) for i in range(2)]
    return list(d), c, total(own, received, rank), rest


def depart(c, sums, transfer_ref, c_ref, out_ref):
    side = side_of(0)
    up = nn(c[0], transfer_ref[0, side]) + nn(c[1], transfer_ref[0, 1 - side])
    for i in range(2):
        c_ref[i] = c[i]
    out_ref[...] = join(up, sums, out_ref.shape[1])


def inverse_end_kernel(column, heights, count, composed, products_ref, link_ref, *refs):
    d, c, totals, rest = head(refs, heights, count, composed, products_ref, link_ref)
    transfer_next, w, *rest = rest
    krylov, rest = rest[:column], rest[column:]
    coefficients, rest = rest[:column], rest[column:]
    d_ref, totals_ref, u_ref, c_ref, out_ref = rest
    totals_ref[...] = totals
    u = [w[0], w[1]]
    if column == 0:
        norm = jnp.sqrt(totals[:, 0:1] + EPSILON)
        u = [x / norm for x in u]
        c = [x / norm for x in c]
        sums = []
    else:
        for i in range(column):
            h = totals[:, i : i + 1]
            for side in range(2):
                u[side] = u[side] - h * krylov[i][side]
                c[side] = c[side] - h * coefficients[i][side]
        sums = [column_sum(u, u)]
    depart(c, sums, transfer_next, c_ref, out_ref)
    for side in range(2):
        d_ref[side] = d[side]
        u_ref[side] = u[side]


def inverse_image_kernel(column, *refs):
    d, ev, rows_own, rows_near, totals, *rest = refs
    images, rest = rest[:column], rest[column:]
    z = [ev[0] + nn(d[0], rows_own[0]), ev[1] + nn(d[1], rows_near[...])]
    if column == 0:
        norm = jnp.sqrt(totals[:, 0:1] + EPSILON)
        z = [x / norm for x in z]
    for i in range(column):
        h = totals[:, i : i + 1]
        for side in range(2):
            z[side] = z[side] - h * images[i][side]
    for side in range(2):
        rest[0][side] = z[side]
    if column == 0:
        rest[1][...] = z[1]


def forward_part_kernel(count, ev, columns_own, columns_near, rows_own, rows_near, *refs):
    basis, (products_ref, sums_ref, b_ref) = refs[:count], refs[count:]
    products_ref[0] = nt(ev[0], columns_own[0])
    products_ref[1] = nt(ev[1], columns_near[...])
    for i, x in enumerate(basis):
        sums_ref[i] = jnp.broadcast_to(column_sum(x, ev), sums_ref.shape[1:])
        b_ref[i, 0] = nt(x[0], rows_own[0])
        b_ref[i, 1] = nt(x[1], rows_near[...])


def inverse_part_kernel(ev, columns_own, columns_near, products_ref):
    products_ref[0] = nt(ev[0], columns_own[0])
    products_ref[1] = nt(ev[1], columns_near[...])


def forward_middle_end_kernel(column, heights, count, composed, products_ref, link_ref, *refs):
    d, c, totals, rest = head(refs, heights, count, composed, products_ref, link_ref)
    transfer_next, sums_in, b, *rest = rest
    if column > 0:
        coefficient, *rest = rest
    d_ref, totals_ref, c_ref, out_ref, *rest = rest
    totals_ref[...] = totals
    sums = []
    for i in range(column + 1):
        part = jnp.sum(b[i, 0] * d[0] + b[i, 1] * d[1], axis=1, keepdims=True)
        sums.append(sums_in[i][:, 0:1] + part)
    if column > 0:
        norm = jnp.sqrt(totals[:, 0:1] + EPSILON)
        c = [x / norm for x in c]
        sums = [x / norm for x in sums]
        sums[-1] = sums[-1] / norm
    depart(c, sums, transfer_next, c_ref, out_ref)
    for side in range(2):
        d_ref[side] = d[side]
        if column > 0:
            rest[0][side] = coefficient[side] / norm


def forward_image_kernel(column, d, ev, rows_own, rows_near, totals, *refs):
    w = [ev[0] + nn(d[0], rows_own[0]), ev[1] + nn(d[1], rows_near[...])]
    if column == 0:
        (w_ref,) = refs
    else:
        u, z, w_ref, q_ref, z_ref, given_ref = refs
        norm = jnp.sqrt(totals[:, 0:1] + EPSILON)
        w = [x / norm for x in w]
        for side in range(2):
            q_ref[side] = u[side] / norm
            z_ref[side] = z[side] / norm
        given_ref[...] = z[1] / norm
    for side in range(2):
        w_ref[side] = w[side]


def link_kernel(rows_own, rows_near, columns_own, columns_near, out_ref):
    pairs = ((rows_own[0], columns_own[0]), (rows_near[...], columns_near[...]))
    m = jnp.concatenate(
        [
            lax.dot_general(p, q, (((1,), (1,)), ((), ())), preferred_element_type=F32)
            for p, q in pairs
        ],
        axis=0,
    )
    size = m.shape[0]
    terms = split3(m)
    for i in range(3):
        out_ref[i] = terms[i * size : (i + 1) * size]


def gram_kernel(*refs):
    *basis, out_ref = refs
    count = len(basis)
    gram, lower, pivots, inverses = {}, {}, [], []
    for i, x in enumerate(basis):
        for k, y in enumerate(basis[: i + 1]):
            gram[i, k] = column_sum(x, y)
    for j in range(count):
        pivot = gram[j, j]
        for k in range(j):
            pivot = pivot - lower[j, k] * lower[j, k] * pivots[k]
        safe = pivot > 1e-6 * gram[j, j]
        inverse = jnp.where(safe, 1.0 / jnp.where(safe, pivot, 1.0), 0.0)
        pivots.append(pivot)
        inverses.append(inverse)
        for i in range(j + 1, count):
            value = gram[i, j]
            for k in range(j):
                value = value - lower[i, k] * lower[j, k] * pivots[k]
            lower[i, j] = value * inverse
    values = [gram[i, k] for i in range(count) for k in range(i + 1)]
    values += [lower[i, k] for i in range(count) for k in range(i)] + inverses
    for i, value in enumerate(values):
        out_ref[i] = jnp.broadcast_to(value, out_ref.shape[1:])


def forward_last_kernel(column, heights, count, composed, *refs):
    values, totals, rest = read(refs, count, composed)
    gram_ref, *rest = rest
    known, rest = rest[: 2 * column], rest[2 * column :]
    w = list(spread(values, heights))
    earlier, rest = rest[:column], rest[column:]
    u_ref, z_ref, z_out_ref, z_given_ref, rows_ref, known_ref = rest
    norm = jnp.sqrt(totals[:, 0:1] + EPSILON)
    q = [u_ref[side] / norm for side in range(2)]
    w = [x / norm for x in w]
    sums = [column_sum(x, w) for x in list(earlier) + [q]]
    rows = last_rows(list(earlier) + [q], w, sums, gram_ref, norm)
    rows_ref[...] = jnp.broadcast_to(rows[None], rows_ref.shape)
    for side in range(2):
        z = z_ref[side] / norm
        z_out_ref[side] = z
    z_given_ref[...] = z
    values = []
    for i in range(2 * column):
        values += [known[i][:, k : k + 1] for k in range((i + 1) // 2 if i % 2 else 1)]
    values.append(totals[:, 0:1])
    known_ref[...] = jnp.transpose(join(None, values, 128))[:SUMS]


def local_projection(lower, inverses, products):
    count = len(products)
    rhs = list(products)
    for j in range(count):
        for k in range(j):
            rhs[j] = rhs[j] - lower[j, k] * rhs[k]
    solved = [rhs[j] * inverses[j] for j in range(count)]
    for j in reversed(range(count)):
        for k in range(j + 1, count):
            solved[j] = solved[j] - lower[k, j] * solved[k]
    return solved


def last_rows(basis, w, products, gram_ref, norm):
    count = len(basis)
    n, leaf = w[0].shape

    def wide(x):
        return jnp.broadcast_to(x, (n, 128))

    norm = wide(norm)
    products = [wide(x) for x in products]
    gram, at = [], 0
    for i in range(count):
        for k in range(i + 1):
            value = gram_ref[at]
            if i + 1 == count:
                value = value / norm
            if k + 1 == count:
                value = value / norm
            gram.append(value)
            at += 1
    lower = {}
    for i in range(count):
        for k in range(i):
            lower[i, k] = gram_ref[at]
            at += 1
    inverses = [gram_ref[at + i] for i in range(count)]
    p = local_projection(lower, inverses, products[:-1] + [products[-1] * norm])
    p[-1] = p[-1] * norm
    t = list(w)
    for i, q in enumerate(basis):
        factor = jnp.concatenate([p[i]] * (leaf // 128), axis=1)
        for side in range(2):
            t[side] = t[side] - factor * q[side]
    values = products + p + [column_sum(t, q) for q in basis] + [column_sum(t, t)] + gram
    rows = jnp.transpose(join(None, values, 128))
    return jnp.concatenate([rows[:SUMS], rows[SUMS : 2 * SUMS]], axis=1)


def tree_sum(parts):
    while len(parts) > 1:
        parts = [
            parts[i] + parts[i + 1] if i + 1 < len(parts) else parts[i]
            for i in range(0, len(parts), 2)
        ]
    return parts[0]


def last_sums(got_ref):
    count = ITERS
    half = got_ref.shape[2] // 2
    parts = []
    for chip in range(got_ref.shape[0] // 2):
        low, high = got_ref[2 * chip], got_ref[2 * chip + 1]
        upper = jnp.concatenate([low[:, :half], high[:, :half]], axis=1)
        lower = jnp.concatenate([low[:, half:], high[:, half:]], axis=1)
        parts.append(jnp.concatenate([upper, lower], axis=0))
    h = tree_sum([part[:count] for part in parts])
    squares = []
    for part in parts:
        e = h - part[count : 2 * count]
        square = part[3 * count : 3 * count + 1]
        at = 3 * count + 1
        for i in range(count):
            row = e[i : i + 1]
            square = square - 2.0 * row * part[2 * count + i : 2 * count + i + 1]
            for k in range(i + 1):
                factor = 1.0 if i == k else 2.0
                square = square + factor * row * e[k : k + 1] * part[at : at + 1]
                at += 1
        squares.append(square)
    return h, jnp.maximum(tree_sum(squares), 0.0)


def columns_of(rows):
    n = rows.shape[1]
    padded = jnp.concatenate([rows, jnp.zeros((128 - rows.shape[0], n), F32)], axis=0)
    return jnp.transpose(padded)


def least_squares(entries, beta_first):
    unknowns = len(entries[0])
    matrix = [list(line) for line in entries]
    target = [beta_first] + [jnp.zeros_like(beta_first) for _ in range(unknowns)]
    for column in range(unknowns):
        upper_entry = matrix[column][column]
        lower_entry = matrix[column + 1][column]
        radius = jnp.sqrt(upper_entry * upper_entry + lower_entry * lower_entry)
        cosine = upper_entry / radius
        sine_value = lower_entry / radius
        for following in range(column, unknowns):
            top_value = matrix[column][following]
            bottom_value = matrix[column + 1][following]
            matrix[column][following] = cosine * top_value + sine_value * bottom_value
            matrix[column + 1][following] = cosine * bottom_value - sine_value * top_value
        top_value = target[column]
        bottom_value = target[column + 1]
        target[column] = cosine * top_value + sine_value * bottom_value
        target[column + 1] = cosine * bottom_value - sine_value * top_value
    coefficients = [None] * unknowns
    for current_row in reversed(range(unknowns)):
        remainder = target[current_row]
        for following in range(current_row + 1, unknowns):
            remainder = remainder - matrix[current_row][following] * coefficients[following]
        coefficients[current_row] = remainder / matrix[current_row][current_row]
    return coefficients


def answer_kernel(got_ref, mine_ref, other_ref, *refs):
    given = refs[:ITERS]
    images = refs[ITERS : 2 * ITERS]
    out_ref, hess_ref = refs[2 * ITERS :]
    even = side_of(0) == 0

    def ordered(own, got, axis):
        return jnp.concatenate(
            [jnp.where(even, own, got), jnp.where(even, got, own)], axis=axis
        )

    known = ordered(mine_ref[...], other_ref[...], 1)
    last, square = last_sums(got_ref)

    def root(x):
        return jnp.sqrt(x + EPSILON)

    row = [known[i : i + 1] for i in range(SUMS)]
    beta = root(row[0])
    zero = jnp.zeros_like(beta)
    entries = [[zero] * ITERS for _ in range(ITERS + 1)]
    at = 1
    for column in range(ITERS - 1):
        for i in range(column + 1):
            entries[i][column] = row[at]
            at += 1
        entries[column + 1][column] = root(row[at])
        at += 1
    for i in range(ITERS):
        entries[i][ITERS - 1] = last[i : i + 1]
    entries[ITERS][ITERS - 1] = root(square)
    y = columns_of(jnp.concatenate(least_squares(entries, beta), axis=0))
    x = None
    for i in range(ITERS):
        term = y[:, i : i + 1] * ordered(images[i][0], given[i][...], 0)
        x = term if x is None else x + term
    out_ref[...] = jnp.transpose(x)
    for i, line in enumerate(entries):
        hess_ref[i] = jnp.concatenate(line, axis=0)


class Operator:
    def __init__(self, tag, blocks, rows, columns, transfer, coupling):
        self.tag = tag
        self.blocks, self.rows, self.columns = blocks, rows, columns
        self.transfer, self.coupling = transfer, coupling
        self.near = {}

    def fetch(self, name, earlier=None):
        if name not in self.near:
            self.near[name] = swapped(getattr(self, name), earlier)
        return getattr(self, name), self.near[name]


def exchange(block, height, levels):
    masks = [1 << height]
    if height + 1 < levels:
        masks += [2 << height, 3 << height]
    return [from_partner(block, mask) for mask in masks]


def stack_kernel(own_ref, near_ref, out_ref):
    out_ref[0] = own_ref[...]
    out_ref[1] = near_ref[...]


def rounds(op, block, c, n, beside):
    levels, _, rank, _ = op.transfer.shape
    width = rank + SUMS
    siblings = []
    h = 1
    unit = 6 * n * rank * rank
    results = None
    while h + 2 < levels:
        received = exchange(block, h, levels)
        if h == 1:
            results = beside(received[0])
            received, results = lax.optimization_barrier((received, results))
        block, sibling = call(
            functools.partial(middle_kernel, h),
            (shape(n * width // 128, 128), shape(2, n, rank)),
            6 * unit,
            block,
            *received,
            op.transfer,
        )
        siblings.append(sibling)
        h += 2
    heights = tuple(range(h, levels))
    received = exchange(block, h, levels)
    if results is None:
        results = beside(received[0])
    cross = call(
        cross_kernel, shape(3, n, rank), (h + 1) * unit, c, *siblings, op.transfer, op.coupling
    )
    return heights, block, received, cross, results


def device_body(
    right_side,
    diag_blocks,
    row_bases,
    column_bases,
    transfer,
    coupling,
    inverse_blocks,
    inverse_rows,
    inverse_columns,
    inverse_transfer,
    inverse_coupling,
):
    inverse = Operator(
        "inverse", inverse_blocks, inverse_rows, inverse_columns, inverse_transfer, inverse_coupling
    )
    forward = Operator("forward", diag_blocks, row_bases, column_bases, transfer, coupling)
    leaf, columns = right_side.shape
    n = columns // 2
    rank = transfer.shape[2]
    width = -(-(rank + SUMS) // 128) * 128
    unit = 6 * n * rank * rank
    big = 6 * n * rank * leaf

    local = pl.BlockSpec(memory_space=pltpu.VMEM)
    away = pl.BlockSpec(memory_space=pltpu.HBM)
    kept, sent, r_kept, r_sent, up = pl.pallas_call(
        first_kernel,
        out_shape=(
            shape(n, width),
            shape(n, width),
            shape(n, leaf),
            shape(n, leaf),
            shape(2, rank, rank, dtype=BF16),
        ),
        in_specs=[away] * 3,
        out_specs=(local,) * 5,
        scratch_shapes=[
            pltpu.VMEM((leaf, columns), F32),
            pltpu.VMEM((rank, leaf), BF16),
            pltpu.SemaphoreType.DMA((4,)),
        ],
        name="first",
        compiler_params=pltpu.CompilerParams(vmem_limit_bytes=VMEM_LIMIT),
    )(
        *[
            pltpu.with_memory_space_constraint(x, pltpu.HBM)
            for x in (right_side, inverse_columns, inverse_transfer)
        ]
    )
    near = with_partner(sent)
    block_shape = shape(n, width)
    pair, vectors, sums_shape = shape(2, n, rank), shape(2, n, leaf), shape(n, SUMS)
    block, c = call(meet_kernel, (block_shape, pair), 2 * unit, kept, near, up)

    def product(op, v):
        e_own, e_near = op.fetch("blocks")
        flops = 12 * n * leaf * leaf
        return call(block_kernel, vectors, flops, v, e_own[0], e_near, scratch=split_scratch)

    def link(op, following):
        out = shape(3, 2 * rank, rank, dtype=BF16)
        operands = (*op.fetch("rows"), *following.fetch("columns"))
        return call(link_kernel, out, 4 * rank * rank * leaf, *operands)

    split_scratch = [pltpu.VMEM((3 * n, leaf), BF16)]
    composites = {}

    def compose(op, heights, earlier):
        composites[op.tag] = call(
            functools.partial(composite_kernel, heights),
            shape(3, (2 * len(heights) - 1) * rank, rank, dtype=BF16),
            20 * rank**3,
            after(op.transfer, earlier),
            op.coupling,
        )

    def exchanged(op, state):
        heights, block, received, cross, _ = state
        operands = (block, *received, cross, op.transfer, op.coupling)
        composed = op.tag in composites
        if composed:
            operands += (composites[op.tag],)
        return operands, (heights, len(received), composed)

    def half_product():
        return call(
            half_block_kernel,
            (shape(n, leaf), shape(n, leaf)),
            12 * n * leaf * leaf,
            r_kept,
            r_sent,
            inverse_blocks,
            scratch=split_scratch,
        )

    krylov, images, coefficients, given, totals = [], [], [], [], []
    links = {}
    for column in range(ITERS):
        last = column + 1 == ITERS
        if column == 0:
            state = rounds(inverse, block, c, n, lambda _: half_product())
            half_kept, half_sent = state[4]
            inverse.fetch("rows", block)
            forward.fetch("columns", block)
            r_near = with_partner(r_sent)
            half_near = with_partner(half_sent)
            w = call(stack_kernel, vectors, n * leaf, r_kept, r_near)
            ev = call(stack_kernel, vectors, n * leaf, half_kept, half_near)
            forward.fetch("blocks", state[1])
            links["inverse"] = link(inverse, forward)
        else:
            state = rounds(inverse, block, c, n, lambda _: product(inverse, w))
            ev = state[4]
        part = call(inverse_part_kernel, pair, big, ev, *forward.fetch("columns"))
        operands, options = exchanged(inverse, state)
        if column == 1:
            compose(forward, state[0], block)
        d, t, u, c, block = call(
            functools.partial(inverse_end_kernel, column, *options),
            (pair, sums_shape, vectors, pair, block_shape),
            4 * big,
            part,
            links["inverse"],
            *operands,
            forward.transfer,
            w,
            *krylov,
            *coefficients,
        )
        totals.append(t)
        z, *z_given = call(
            functools.partial(inverse_image_kernel, column),
            (vectors,) + ((shape(n, leaf),) if column == 0 else ()),
            2 * big,
            d,
            ev,
            *inverse.fetch("rows"),
            t,
            *images,
        )
        if column == 0:
            given += z_given
            images.append(z)
            krylov.append(u)
            coefficients.append(c)
            forward.fetch("rows", u)
            inverse.fetch("columns", u)
            links["forward"] = link(forward, inverse)
        state = rounds(forward, block, c, n, lambda _: product(forward, z))
        ev = state[4]
        if column == 0:
            inverse.fetch("blocks", state[1])
        operands, options = exchanged(forward, state)
        if column == 0:
            compose(inverse, state[0], block)
        basis = krylov if column == 0 else krylov + [u]
        count = len(basis)
        if last:
            out = shape(count * (count + 1), n, 128)
            gram = call(gram_kernel, out, big, *basis)
            p_own, p_near = forward.fetch("rows")
            _, block, received, cross, _ = state
            tail = operands[2 + len(received) :]
            z, z_given, rows, known = call(
                functools.partial(forward_last_kernel, column, *options),
                (
                    vectors,
                    shape(n, leaf),
                    shape(lax.axis_size("leaf"), SUMS, 2 * n),
                    shape(SUMS, n),
                ),
                4 * big,
                block,
                *received,
                cross,
                ev,
                p_own,
                p_near,
                *tail,
                gram,
                *totals,
                *krylov,
                u,
                z,
            )
            images.append(z)
            given.append(z_given)
            break
        part, sums, b = call(
            functools.partial(forward_part_kernel, count),
            (pair, shape(count, n, 128), shape(count, 2, n, rank)),
            (1 + count) * big,
            ev,
            *inverse.fetch("columns"),
            *forward.fetch("rows"),
            *basis,
        )
        outs = [pair, sums_shape, pair, block_shape] + ([] if column == 0 else [pair])
        d, t, c_next, block, *coefficient = call(
            functools.partial(forward_middle_end_kernel, column, *options),
            tuple(outs),
            4 * big,
            part,
            links["forward"],
            *operands,
            inverse.transfer,
            sums,
            b,
            *([] if column == 0 else [c]),
        )
        outs = [vectors] + ([] if column == 0 else [vectors, vectors, shape(n, leaf)])
        result = call(
            functools.partial(forward_image_kernel, column),
            tuple(outs),
            2 * big,
            d,
            ev,
            *forward.fetch("rows"),
            t,
            *([] if column == 0 else [u, z]),
        )
        w = result[0]
        if column > 0:
            krylov.append(result[1])
            images.append(result[2])
            given.append(result[3])
            coefficients.append(coefficient[0])
            totals.append(t)
        c = c_next

    got = lax.all_to_all(rows, "leaf", 0, 0)
    x, hess = call(
        answer_kernel,
        (shape(leaf, columns), shape(ITERS + 1, ITERS, columns)),
        big,
        got,
        known,
        with_partner(known),
        *[with_partner(z) for z in given],
        *images,
    )
    return (x, hess)


def solution(mesh):
    in_specs = (
        P("leaf", None),
        P("leaf", None, None),
        P("leaf", None, None),
        P("leaf", None, None),
        P(),
        P(),
        P("leaf", None, None),
        P("leaf", None, None),
        P("leaf", None, None),
        P(),
        P(),
    )
    out_specs = (P("leaf", None), P())
    return jax.shard_map(
        device_body, mesh=mesh, in_specs=in_specs, out_specs=out_specs, check_vma=False
    )
```

```python
import functools

import jax
import jax.numpy as jnp
from jax import lax
from jax.experimental import pallas as pl
from jax.experimental.pallas import tpu as pltpu
from jax.sharding import PartitionSpec as P

ITERS = 3
EPSILON = 1e-06
SUMS = 8
VMEM_LIMIT = 12 << 20
F32 = jnp.float32
BF16 = jnp.bfloat16


def from_partner(block, mask):
    count = lax.axis_size("leaf")
    return lax.ppermute(block, "leaf", [(i, i ^ mask) for i in range(count)])


def with_partner(block):
    return from_partner(block, 1)


def shape(*dims, dtype=F32):
    return jax.ShapeDtypeStruct(dims, dtype)


def call(kernel, out, flops, *args, scratch=()):
    local = pl.BlockSpec(memory_space=pltpu.VMEM)
    return pl.pallas_call(
        kernel,
        out_shape=out,
        in_specs=[local] * len(args),
        out_specs=jax.tree.map(lambda _: local, out),
        scratch_shapes=scratch,
        compiler_params=pltpu.CompilerParams(vmem_limit_bytes=VMEM_LIMIT),
        cost_estimate=pl.CostEstimate(flops=flops, bytes_accessed=flops // 512, transcendentals=0),
    )(*args)


def after(values, earlier):
    return lax.optimization_barrier((values, earlier))[0]


def split3(x):
    high = x.astype(BF16)
    rest = x - high.astype(F32)
    middle = rest.astype(BF16)
    low = (rest - middle.astype(F32)).astype(BF16)
    return jnp.concatenate([high, middle, low], axis=0)


def times(x, matrix, contract):
    n = x.shape[0]
    y = lax.dot_general(
        split3(x), matrix, (((1,), (contract,)), ((), ())), preferred_element_type=F32
    )
    return y[:n] + (y[n : 2 * n] + y[2 * n :])


def nn(x, matrix):
    return times(x, matrix, 0)


def nt(x, matrix):
    return times(x, matrix, 1)


def side_of(height):
    return lax.axis_index("leaf") >> height & 1


def crossed_bits():
    levels = lax.axis_size("leaf").bit_length() - 1
    return range(1, min(3, levels))


def half_of():
    half = side_of(0)
    for bit in crossed_bits():
        half = half ^ side_of(bit)
    return half


def join(c, sums, width):
    if c is None:
        n, rank = sums[0].shape[0], 0
        block = jnp.zeros((n, width), F32)
    else:
        n, rank = c.shape
        block = jnp.concatenate([c, jnp.zeros((n, width - rank), F32)], axis=1)
    lane = lax.broadcasted_iota(jnp.int32, (n, width), 1)
    for i, s in enumerate(sums):
        block = jnp.where(lane == rank + i, s, block)
    return block


def padded(block):
    n, width = block.shape
    return jnp.concatenate([block, jnp.zeros((n, -width % 128), F32)], axis=1)


def chunks(width):
    full = width // 128 * 128
    sizes, bit = [], 64
    while bit >= 1:
        if (width - full) & bit:
            sizes.append(bit)
        bit //= 2
    return full, sizes


def pack(block):
    n, width = block.shape
    full, sizes = chunks(width)
    parts = [block[:, at : at + 128] for at in range(0, full, 128)]
    at = full
    for size in sizes:
        rows = n * size // 128
        piece = block[:, at : at + size]
        parts.append(
            jnp.concatenate([piece[i : i + rows] for i in range(0, n, rows)], axis=1)
        )
        at += size
    return jnp.concatenate(parts, axis=0)


def unpack(packed, width):
    if packed.shape[1] > 128:
        return packed[:, :width]
    n = packed.shape[0] * 128 // width
    full, sizes = chunks(width)
    parts, at = [], 0
    for _ in range(0, full, 128):
        parts.append(packed[at : at + n])
        at += n
    for size in sizes:
        rows = n * size // 128
        piece = packed[at : at + rows]
        parts.append(
            jnp.concatenate([piece[:, i : i + size] for i in range(0, 128, size)], axis=0)
        )
        at += rows
    return jnp.concatenate(parts, axis=1)


def first_kernel(
    r_ref, columns_ref, transfer_ref, kept_ref, sent_ref, r_kept_ref, r_sent_ref, up_ref,
    r_local, columns_local, done
):
    side = side_of(0)
    copies = [
        pltpu.make_async_copy(r_ref, r_local, done.at[0]),
        pltpu.make_async_copy(columns_ref.at[0], columns_local, done.at[1]),
        pltpu.make_async_copy(transfer_ref.at[0, side], up_ref.at[0], done.at[2]),
        pltpu.make_async_copy(transfer_ref.at[0, 1 - side], up_ref.at[1], done.at[3]),
    ]
    for copy in copies:
        copy.start()
    copies[0].wait()
    rt = jnp.transpose(r_local[...])
    half = rt.shape[0] // 2
    even = half_of() == 0
    r_kept_ref[...] = jnp.where(even, rt[:half], rt[half:])
    r_sent_ref[...] = jnp.where(even, rt[half:], rt[:half])
    squares = jnp.sum(rt * rt, axis=1, keepdims=True)
    copies[1].wait()
    full = join(nt(rt, columns_local[...]), [squares], kept_ref.shape[1])
    kept_ref[...] = jnp.where(even, full[:half], full[half:])
    sent_ref[...] = jnp.where(even, full[half:], full[:half])
    copies[2].wait()
    copies[3].wait()


def meet_kernel(own_ref, near_ref, up_ref, out_ref, c_ref):
    rank = up_ref.shape[2]
    c_ref[0] = own_ref[:, :rank]
    c_ref[1] = near_ref[:, :rank]
    c = nn(c_ref[0], up_ref[0]) + nn(c_ref[1], up_ref[1])
    sums = own_ref[:, rank : rank + SUMS] + near_ref[:, rank : rank + SUMS]
    out_ref[...] = padded(jnp.concatenate([c, sums], axis=1))


def total(own, received, rank):
    sums = [x[:, rank:] for x in [own] + received]
    if len(sums) == 2:
        return sums[0] + sums[1]
    return (sums[0] + sums[1]) + (sums[2] + sums[3])


def climb(own, received, rank, height, transfer_ref):
    side = side_of(height)
    first, second, third = received
    even = jnp.concatenate([own[:, :rank], second[:, :rank]], axis=0)
    odd = jnp.concatenate([first[:, :rank], third[:, :rank]], axis=0)
    return nn(even, transfer_ref[height, side]) + nn(odd, transfer_ref[height, 1 - side])


def middle_kernel(height, own_ref, a_ref, b_ref, ab_ref, transfer_ref, out_ref, sibling_ref):
    rank = transfer_ref.shape[2]
    width = rank + SUMS
    own, *received = [unpack(x[...], width) for x in (own_ref, a_ref, b_ref, ab_ref)]
    n = own.shape[0]
    both = climb(own, received, rank, height, transfer_ref)
    side = side_of(height + 1)
    c = nn(both[:n], transfer_ref[height + 1, side])
    c = c + nn(both[n:], transfer_ref[height + 1, 1 - side])
    out_ref[...] = pack(jnp.concatenate([c, total(own, received, rank)], axis=1))
    sibling_ref[0] = received[0][:, :rank]
    sibling_ref[1] = both[n:]


def cross_kernel(c_ref, *refs):
    *siblings, transfer_ref, coupling_ref, out_ref = refs
    side = side_of(0)
    out_ref[0] = nt(c_ref[1], coupling_ref[0, side])
    out_ref[1] = nt(c_ref[0], coupling_ref[0, 1 - side])
    d = None
    for h in reversed(range(1, 2 * len(siblings) + 1)):
        term = nt(siblings[(h - 1) // 2][(h - 1) % 2], coupling_ref[h, side_of(h)])
        d = term if d is None else term + nt(d, transfer_ref[h, side_of(h)])
    out_ref[2] = jnp.zeros(out_ref.shape[1:], F32) if d is None else d


def block_rows(v_ref, matrix_ref, out_ref, split_ref):
    n, leaf = v_ref.shape
    chunk = leaf
    split_ref[...] = split3(v_ref[...])

    def step(i, carry):
        at = pl.multiple_of(i * chunk, chunk)
        y = lax.dot_general(
            split_ref[...],
            matrix_ref[pl.ds(at, chunk)],
            (((1,), (1,)), ((), ())),
            preferred_element_type=F32,
        )
        out_ref[:, pl.ds(at, chunk)] = y[:n] + (y[n : 2 * n] + y[2 * n :])
        return carry

    lax.fori_loop(0, leaf // chunk, step, 0)


def half_block_kernel(kept_ref, sent_ref, own_ref, out_kept_ref, out_sent_ref, split_ref):
    block_rows(kept_ref, own_ref.at[0], out_kept_ref, split_ref)
    block_rows(sent_ref, own_ref.at[0], out_sent_ref, split_ref)


def block_kernel(v_ref, own_ref, near_ref, out_ref, split_ref):
    block_rows(v_ref.at[0], own_ref, out_ref.at[0], split_ref)
    block_rows(v_ref.at[1], near_ref, out_ref.at[1], split_ref)


def widen_kernel(x_ref, out_ref):
    out_ref[...] = x_ref[0].astype(F32)


def narrow_kernel(x_ref, out_ref):
    out_ref[...] = x_ref[...].astype(BF16)


def swapped(matrix, earlier):
    rows, columns = matrix.shape[1:]
    matrix = after(matrix, earlier)
    wide = call(widen_kernel, shape(rows, columns), rows * columns, matrix)
    wide = with_partner(wide)
    return call(narrow_kernel, shape(rows, columns, dtype=BF16), rows * columns, wide)


def composite_kernel(heights, transfer_ref, coupling_ref, out_ref):
    rank = transfer_ref.shape[2]
    low = heights[0]
    side = side_of(low)
    row = lax.broadcasted_iota(jnp.int32, (rank, rank), 0)
    lane = lax.broadcasted_iota(jnp.int32, (rank, rank), 1)
    m = nt(jnp.where(row == lane, 1.0, 0.0).astype(F32), coupling_ref[low, side])
    if len(heights) == 2:
        high = heights[1]
        rest = jnp.concatenate(
            [transfer_ref[low, side].astype(F32), transfer_ref[low, 1 - side].astype(F32)], axis=0
        )
        rest = nt(rest, coupling_ref[high, side_of(high)])
        m = jnp.concatenate([m, nt(rest, transfer_ref[low, side])], axis=0)
    for h in reversed(range(1, low)):
        m = nt(m, transfer_ref[h, side_of(h)])
    size = m.shape[0]
    terms = split3(m)
    for i in range(3):
        out_ref[i] = terms[i * size : (i + 1) * size]


def through(x, composite_ref, at):
    n, rank = x.shape
    terms = split3(x)
    result = None
    for i in reversed(range(3)):
        matrix = composite_ref[i, at : at + rank]
        y = jnp.dot(terms[: (3 - i) * n], matrix, preferred_element_type=F32)
        for k in reversed(range(3 - i)):
            part = y[k * n : (k + 1) * n]
            result = part if result is None else result + part
    return result


def descend(heights, received, cross, transfer_ref, coupling_ref, composite_ref):
    rank = transfer_ref.shape[2]
    low = heights[0]
    if composite_ref is not None:
        d = None
        blocks = received if len(heights) == 2 else received[:1]
        for i, block in enumerate(blocks):
            part = through(block[:, :rank], composite_ref, i * rank)
            d = part if d is None else d + part
    else:
        side = side_of(low)
        d = nt(received[0][:, :rank], coupling_ref[low, side])
        if len(heights) == 2:
            high = heights[1]
            even, odd = received[1][:, :rank], received[2][:, :rank]
            sibling = nn(even, transfer_ref[low, side]) + nn(odd, transfer_ref[low, 1 - side])
            top = nt(sibling, coupling_ref[high, side_of(high)])
            d = d + nt(top, transfer_ref[low, side])
        for h in reversed(range(1, low)):
            d = nt(d, transfer_ref[h, side_of(h)])
    d = cross[2] + d
    side = side_of(0)
    d_own = cross[0] + nt(d, transfer_ref[0, side])
    d_near = cross[1] + nt(d, transfer_ref[0, 1 - side])
    return d_own, d_near


def spread(values, heights):
    received, cross, blocks, rows_own, rows_near, transfer, coupling, composite = values
    d_own, d_near = descend(heights, received, cross, transfer, coupling, composite)
    return blocks[0] + nn(d_own, rows_own), blocks[1] + nn(d_near, rows_near)


def column_sum(x, y):
    return jnp.sum(x[0] * y[0] + x[1] * y[1], axis=1, keepdims=True)


def read(refs, received_count, composed):
    cross, blocks, rows_own, rows_near, transfer, coupling = refs[
        1 + received_count : 7 + received_count
    ]
    rest = refs[7 + received_count :]
    composite = None
    if composed:
        composite, *rest = rest
    rank = transfer.shape[2]
    own, *received = [unpack(r[...], rank + SUMS) for r in refs[: 1 + received_count]]
    values = (
        received, cross, blocks, rows_own[0], rows_near[...], transfer, coupling, composite
    )
    return values, total(own, received, rank), rest


def head(refs, heights, count, composed, products_ref, link_ref):
    cross, transfer, coupling = refs[1 + count : 4 + count]
    rest = refs[4 + count :]
    composite = None
    if composed:
        composite, *rest = rest
    rank = transfer.shape[2]
    own, *received = [unpack(r[...], rank + SUMS) for r in refs[: 1 + count]]
    d = descend(heights, received, cross, transfer, coupling, composite)
    c = [products_ref[i] + through(d[i], link_ref, i * rank) for i in range(2)]
    return list(d), c, total(own, received, rank), rest


def depart(c, sums, transfer_ref, c_ref, out_ref):
    side = side_of(0)
    up = nn(c[0], transfer_ref[0, side]) + nn(c[1], transfer_ref[0, 1 - side])
    for i in range(2):
        c_ref[i] = c[i]
    out_ref[...] = join(up, sums, out_ref.shape[1])


def inverse_end_kernel(column, heights, count, composed, products_ref, link_ref, *refs):
    d, c, totals, rest = head(refs, heights, count, composed, products_ref, link_ref)
    transfer_next, w, *rest = rest
    krylov, rest = rest[:column], rest[column:]
    coefficients, rest = rest[:column], rest[column:]
    d_ref, totals_ref, u_ref, c_ref, out_ref = rest
    totals_ref[...] = totals
    u = [w[0], w[1]]
    if column == 0:
        norm = jnp.sqrt(totals[:, 0:1] + EPSILON)
        u = [x / norm for x in u]
        c = [x / norm for x in c]
        sums = []
    else:
        for i in range(column):
            h = totals[:, i : i + 1]
            for side in range(2):
                u[side] = u[side] - h * krylov[i][side]
                c[side] = c[side] - h * coefficients[i][side]
        sums = [column_sum(u, u)]
    depart(c, sums, transfer_next, c_ref, out_ref)
    for side in range(2):
        d_ref[side] = d[side]
        u_ref[side] = u[side]


def inverse_image_kernel(column, *refs):
    d, ev, rows_own, rows_near, totals, *rest = refs
    images, rest = rest[:column], rest[column:]
    z = [ev[0] + nn(d[0], rows_own[0]), ev[1] + nn(d[1], rows_near[...])]
    if column == 0:
        norm = jnp.sqrt(totals[:, 0:1] + EPSILON)
        z = [x / norm for x in z]
    for i in range(column):
        h = totals[:, i : i + 1]
        for side in range(2):
            z[side] = z[side] - h * images[i][side]
    for side in range(2):
        rest[0][side] = z[side]
    if column == 0:
        rest[1][...] = z[1]


def forward_part_kernel(count, ev, columns_own, columns_near, rows_own, rows_near, *refs):
    basis, (products_ref, sums_ref, b_ref) = refs[:count], refs[count:]
    products_ref[0] = nt(ev[0], columns_own[0])
    products_ref[1] = nt(ev[1], columns_near[...])
    for i, x in enumerate(basis):
        sums_ref[i] = jnp.broadcast_to(column_sum(x, ev), sums_ref.shape[1:])
        b_ref[i, 0] = nt(x[0], rows_own[0])
        b_ref[i, 1] = nt(x[1], rows_near[...])


def inverse_part_kernel(ev, columns_own, columns_near, products_ref):
    products_ref[0] = nt(ev[0], columns_own[0])
    products_ref[1] = nt(ev[1], columns_near[...])


def forward_middle_end_kernel(column, heights, count, composed, products_ref, link_ref, *refs):
    d, c, totals, rest = head(refs, heights, count, composed, products_ref, link_ref)
    transfer_next, sums_in, b, *rest = rest
    if column > 0:
        coefficient, *rest = rest
    d_ref, totals_ref, c_ref, out_ref, *rest = rest
    totals_ref[...] = totals
    sums = []
    for i in range(column + 1):
        part = jnp.sum(b[i, 0] * d[0] + b[i, 1] * d[1], axis=1, keepdims=True)
        sums.append(sums_in[i][:, 0:1] + part)
    if column > 0:
        norm = jnp.sqrt(totals[:, 0:1] + EPSILON)
        c = [x / norm for x in c]
        sums = [x / norm for x in sums]
        sums[-1] = sums[-1] / norm
    depart(c, sums, transfer_next, c_ref, out_ref)
    for side in range(2):
        d_ref[side] = d[side]
        if column > 0:
            rest[0][side] = coefficient[side] / norm


def forward_image_kernel(column, d, ev, rows_own, rows_near, totals, *refs):
    w = [ev[0] + nn(d[0], rows_own[0]), ev[1] + nn(d[1], rows_near[...])]
    if column == 0:
        (w_ref,) = refs
    else:
        u, z, w_ref, q_ref, z_ref, given_ref = refs
        norm = jnp.sqrt(totals[:, 0:1] + EPSILON)
        w = [x / norm for x in w]
        for side in range(2):
            q_ref[side] = u[side] / norm
            z_ref[side] = z[side] / norm
        given_ref[...] = z[1] / norm
    for side in range(2):
        w_ref[side] = w[side]


def link_kernel(rows_own, rows_near, columns_own, columns_near, out_ref):
    pairs = ((rows_own[0], columns_own[0]), (rows_near[...], columns_near[...]))
    m = jnp.concatenate(
        [
            lax.dot_general(p, q, (((1,), (1,)), ((), ())), preferred_element_type=F32)
            for p, q in pairs
        ],
        axis=0,
    )
    size = m.shape[0]
    terms = split3(m)
    for i in range(3):
        out_ref[i] = terms[i * size : (i + 1) * size]


def gram_kernel(*refs):
    *basis, out_ref = refs
    count = len(basis)
    gram, lower, pivots, inverses = {}, {}, [], []
    for i, x in enumerate(basis):
        for k, y in enumerate(basis[: i + 1]):
            gram[i, k] = column_sum(x, y)
    for j in range(count):
        pivot = gram[j, j]
        for k in range(j):
            pivot = pivot - lower[j, k] * lower[j, k] * pivots[k]
        safe = pivot > 1e-6 * gram[j, j]
        inverse = jnp.where(safe, 1.0 / jnp.where(safe, pivot, 1.0), 0.0)
        pivots.append(pivot)
        inverses.append(inverse)
        for i in range(j + 1, count):
            value = gram[i, j]
            for k in range(j):
                value = value - lower[i, k] * lower[j, k] * pivots[k]
            lower[i, j] = value * inverse
    values = [gram[i, k] for i in range(count) for k in range(i + 1)]
    values += [lower[i, k] for i in range(count) for k in range(i)] + inverses
    for i, value in enumerate(values):
        out_ref[i] = jnp.broadcast_to(value, out_ref.shape[1:])


def forward_last_kernel(column, heights, count, composed, *refs):
    values, totals, rest = read(refs, count, composed)
    gram_ref, *rest = rest
    known, rest = rest[: 2 * column], rest[2 * column :]
    w = list(spread(values, heights))
    earlier, rest = rest[:column], rest[column:]
    u_ref, z_ref, z_out_ref, z_given_ref, rows_ref, known_ref = rest
    norm = jnp.sqrt(totals[:, 0:1] + EPSILON)
    q = [u_ref[side] / norm for side in range(2)]
    w = [x / norm for x in w]
    sums = [column_sum(x, w) for x in list(earlier) + [q]]
    rows = last_rows(list(earlier) + [q], w, sums, gram_ref, norm)
    rows_ref[...] = jnp.broadcast_to(rows[None], rows_ref.shape)
    for side in range(2):
        z = z_ref[side] / norm
        z_out_ref[side] = z
    z_given_ref[...] = z
    values = []
    for i in range(2 * column):
        values += [known[i][:, k : k + 1] for k in range((i + 1) // 2 if i % 2 else 1)]
    values.append(totals[:, 0:1])
    known_ref[...] = jnp.transpose(join(None, values, 128))[:SUMS]


def local_projection(lower, inverses, products):
    count = len(products)
    rhs = list(products)
    for j in range(count):
        for k in range(j):
            rhs[j] = rhs[j] - lower[j, k] * rhs[k]
    solved = [rhs[j] * inverses[j] for j in range(count)]
    for j in reversed(range(count)):
        for k in range(j + 1, count):
            solved[j] = solved[j] - lower[k, j] * solved[k]
    return solved


def last_rows(basis, w, products, gram_ref, norm):
    count = len(basis)
    n, leaf = w[0].shape

    def wide(x):
        return jnp.broadcast_to(x, (n, 128))

    norm = wide(norm)
    products = [wide(x) for x in products]
    gram, at = [], 0
    for i in range(count):
        for k in range(i + 1):
            value = gram_ref[at]
            if i + 1 == count:
                value = value / norm
            if k + 1 == count:
                value = value / norm
            gram.append(value)
            at += 1
    lower = {}
    for i in range(count):
        for k in range(i):
            lower[i, k] = gram_ref[at]
            at += 1
    inverses = [gram_ref[at + i] for i in range(count)]
    p = local_projection(lower, inverses, products[:-1] + [products[-1] * norm])
    p[-1] = p[-1] * norm
    t = list(w)
    for i, q in enumerate(basis):
        factor = jnp.concatenate([p[i]] * (leaf // 128), axis=1)
        for side in range(2):
            t[side] = t[side] - factor * q[side]
    values = products + p + [column_sum(t, q) for q in basis] + [column_sum(t, t)] + gram
    rows = jnp.transpose(join(None, values, 128))
    return jnp.concatenate([rows[:SUMS], rows[SUMS : 2 * SUMS]], axis=1)


def tree_sum(parts):
    while len(parts) > 1:
        parts = [
            parts[i] + parts[i + 1] if i + 1 < len(parts) else parts[i]
            for i in range(0, len(parts), 2)
        ]
    return parts[0]


def last_sums(got_ref):
    count = ITERS
    half = got_ref.shape[2] // 2
    parts = []
    for chip in range(got_ref.shape[0] // 2):
        swap = 0
        for bit in crossed_bits():
            swap ^= chip >> (bit - 1) & 1
        low, high = got_ref[2 * chip + swap], got_ref[2 * chip + 1 - swap]
        upper = jnp.concatenate([low[:, :half], high[:, :half]], axis=1)
        lower = jnp.concatenate([low[:, half:], high[:, half:]], axis=1)
        parts.append(jnp.concatenate([upper, lower], axis=0))
    h = tree_sum([part[:count] for part in parts])
    squares = []
    for part in parts:
        e = h - part[count : 2 * count]
        square = part[3 * count : 3 * count + 1]
        at = 3 * count + 1
        for i in range(count):
            row = e[i : i + 1]
            square = square - 2.0 * row * part[2 * count + i : 2 * count + i + 1]
            for k in range(i + 1):
                factor = 1.0 if i == k else 2.0
                square = square + factor * row * e[k : k + 1] * part[at : at + 1]
                at += 1
        squares.append(square)
    return h, jnp.maximum(tree_sum(squares), 0.0)


def columns_of(rows):
    n = rows.shape[1]
    padded = jnp.concatenate([rows, jnp.zeros((128 - rows.shape[0], n), F32)], axis=0)
    return jnp.transpose(padded)


def least_squares(entries, beta_first):
    unknowns = len(entries[0])
    matrix = [list(line) for line in entries]
    target = [beta_first] + [jnp.zeros_like(beta_first) for _ in range(unknowns)]
    for column in range(unknowns):
        upper_entry = matrix[column][column]
        lower_entry = matrix[column + 1][column]
        radius = jnp.sqrt(upper_entry * upper_entry + lower_entry * lower_entry)
        cosine = upper_entry / radius
        sine_value = lower_entry / radius
        for following in range(column, unknowns):
            top_value = matrix[column][following]
            bottom_value = matrix[column + 1][following]
            matrix[column][following] = cosine * top_value + sine_value * bottom_value
            matrix[column + 1][following] = cosine * bottom_value - sine_value * top_value
        top_value = target[column]
        bottom_value = target[column + 1]
        target[column] = cosine * top_value + sine_value * bottom_value
        target[column + 1] = cosine * bottom_value - sine_value * top_value
    coefficients = [None] * unknowns
    for current_row in reversed(range(unknowns)):
        remainder = target[current_row]
        for following in range(current_row + 1, unknowns):
            remainder = remainder - matrix[current_row][following] * coefficients[following]
        coefficients[current_row] = remainder / matrix[current_row][current_row]
    return coefficients


def answer_kernel(got_ref, mine_ref, other_ref, *refs):
    given = refs[:ITERS]
    images = refs[ITERS : 2 * ITERS]
    out_ref, hess_ref = refs[2 * ITERS :]
    even = half_of() == 0

    def ordered(own, got, axis):
        return jnp.concatenate(
            [jnp.where(even, own, got), jnp.where(even, got, own)], axis=axis
        )

    known = ordered(mine_ref[...], other_ref[...], 1)
    last, square = last_sums(got_ref)

    def root(x):
        return jnp.sqrt(x + EPSILON)

    row = [known[i : i + 1] for i in range(SUMS)]
    beta = root(row[0])
    zero = jnp.zeros_like(beta)
    entries = [[zero] * ITERS for _ in range(ITERS + 1)]
    at = 1
    for column in range(ITERS - 1):
        for i in range(column + 1):
            entries[i][column] = row[at]
            at += 1
        entries[column + 1][column] = root(row[at])
        at += 1
    for i in range(ITERS):
        entries[i][ITERS - 1] = last[i : i + 1]
    entries[ITERS][ITERS - 1] = root(square)
    y = columns_of(jnp.concatenate(least_squares(entries, beta), axis=0))
    x = None
    for i in range(ITERS):
        term = y[:, i : i + 1] * ordered(images[i][0], given[i][...], 0)
        x = term if x is None else x + term
    out_ref[...] = jnp.transpose(x)
    for i, line in enumerate(entries):
        hess_ref[i] = jnp.concatenate(line, axis=0)


class Operator:
    def __init__(self, tag, blocks, rows, columns, transfer, coupling):
        self.tag = tag
        self.blocks, self.rows, self.columns = blocks, rows, columns
        self.transfer, self.coupling = transfer, coupling
        self.near = {}

    def fetch(self, name, earlier=None):
        if name not in self.near:
            self.near[name] = swapped(getattr(self, name), earlier)
        return getattr(self, name), self.near[name]


def exchange(block, height, levels):
    cross = 1 if height == 1 else 0
    masks = [1 << height | cross]
    if height + 1 < levels:
        masks += [2 << height | cross, 3 << height]
    return [from_partner(block, mask) for mask in masks]


def stack_kernel(own_ref, near_ref, out_ref):
    out_ref[0] = own_ref[...]
    out_ref[1] = near_ref[...]


def rounds(op, block, c, n, beside):
    levels, _, rank, _ = op.transfer.shape
    width = rank + SUMS
    siblings = []
    h = 1
    unit = 6 * n * rank * rank
    results = None
    while h + 2 < levels:
        received = exchange(block, h, levels)
        if h == 1:
            results = beside(received[0])
            received, results = lax.optimization_barrier((received, results))
        block, sibling = call(
            functools.partial(middle_kernel, h),
            (shape(n * width // 128, 128), shape(2, n, rank)),
            6 * unit,
            block,
            *received,
            op.transfer,
        )
        siblings.append(sibling)
        h += 2
    heights = tuple(range(h, levels))
    received = exchange(block, h, levels)
    if results is None:
        results = beside(received[0])
    cross = call(
        cross_kernel, shape(3, n, rank), (h + 1) * unit, c, *siblings, op.transfer, op.coupling
    )
    return heights, block, received, cross, results


def device_body(
    right_side,
    diag_blocks,
    row_bases,
    column_bases,
    transfer,
    coupling,
    inverse_blocks,
    inverse_rows,
    inverse_columns,
    inverse_transfer,
    inverse_coupling,
):
    inverse = Operator(
        "inverse", inverse_blocks, inverse_rows, inverse_columns, inverse_transfer, inverse_coupling
    )
    forward = Operator("forward", diag_blocks, row_bases, column_bases, transfer, coupling)
    leaf, columns = right_side.shape
    n = columns // 2
    rank = transfer.shape[2]
    width = -(-(rank + SUMS) // 128) * 128
    unit = 6 * n * rank * rank
    big = 6 * n * rank * leaf

    local = pl.BlockSpec(memory_space=pltpu.VMEM)
    away = pl.BlockSpec(memory_space=pltpu.HBM)
    kept, sent, r_kept, r_sent, up = pl.pallas_call(
        first_kernel,
        out_shape=(
            shape(n, width),
            shape(n, width),
            shape(n, leaf),
            shape(n, leaf),
            shape(2, rank, rank, dtype=BF16),
        ),
        in_specs=[away] * 3,
        out_specs=(local,) * 5,
        scratch_shapes=[
            pltpu.VMEM((leaf, columns), F32),
            pltpu.VMEM((rank, leaf), BF16),
            pltpu.SemaphoreType.DMA((4,)),
        ],
        name="first",
        compiler_params=pltpu.CompilerParams(vmem_limit_bytes=VMEM_LIMIT),
    )(
        *[
            pltpu.with_memory_space_constraint(x, pltpu.HBM)
            for x in (right_side, inverse_columns, inverse_transfer)
        ]
    )
    near = with_partner(sent)
    block_shape = shape(n, width)
    pair, vectors, sums_shape = shape(2, n, rank), shape(2, n, leaf), shape(n, SUMS)
    block, c = call(meet_kernel, (block_shape, pair), 2 * unit, kept, near, up)

    def product(op, v):
        e_own, e_near = op.fetch("blocks")
        flops = 12 * n * leaf * leaf
        return call(block_kernel, vectors, flops, v, e_own[0], e_near, scratch=split_scratch)

    def link(op, following):
        out = shape(3, 2 * rank, rank, dtype=BF16)
        operands = (*op.fetch("rows"), *following.fetch("columns"))
        return call(link_kernel, out, 4 * rank * rank * leaf, *operands)

    split_scratch = [pltpu.VMEM((3 * n, leaf), BF16)]
    composites = {}

    def compose(op, heights, earlier):
        composites[op.tag] = call(
            functools.partial(composite_kernel, heights),
            shape(3, (2 * len(heights) - 1) * rank, rank, dtype=BF16),
            20 * rank**3,
            after(op.transfer, earlier),
            op.coupling,
        )

    def exchanged(op, state):
        heights, block, received, cross, _ = state
        operands = (block, *received, cross, op.transfer, op.coupling)
        composed = op.tag in composites
        if composed:
            operands += (composites[op.tag],)
        return operands, (heights, len(received), composed)

    def half_product():
        return call(
            half_block_kernel,
            (shape(n, leaf), shape(n, leaf)),
            12 * n * leaf * leaf,
            r_kept,
            r_sent,
            inverse_blocks,
            scratch=split_scratch,
        )

    krylov, images, coefficients, given, totals = [], [], [], [], []
    links = {}
    for column in range(ITERS):
        last = column + 1 == ITERS
        if column == 0:
            state = rounds(inverse, block, c, n, lambda _: half_product())
            half_kept, half_sent = state[4]
            inverse.fetch("rows", block)
            forward.fetch("columns", block)
            r_near = with_partner(r_sent)
            half_near = with_partner(half_sent)
            w = call(stack_kernel, vectors, n * leaf, r_kept, r_near)
            ev = call(stack_kernel, vectors, n * leaf, half_kept, half_near)
            forward.fetch("blocks", state[1])
            links["inverse"] = link(inverse, forward)
        else:
            state = rounds(inverse, block, c, n, lambda _: product(inverse, w))
            ev = state[4]
        part = call(inverse_part_kernel, pair, big, ev, *forward.fetch("columns"))
        operands, options = exchanged(inverse, state)
        if column == 1:
            compose(forward, state[0], block)
        d, t, u, c, block = call(
            functools.partial(inverse_end_kernel, column, *options),
            (pair, sums_shape, vectors, pair, block_shape),
            4 * big,
            part,
            links["inverse"],
            *operands,
            forward.transfer,
            w,
            *krylov,
            *coefficients,
        )
        totals.append(t)
        z, *z_given = call(
            functools.partial(inverse_image_kernel, column),
            (vectors,) + ((shape(n, leaf),) if column == 0 else ()),
            2 * big,
            d,
            ev,
            *inverse.fetch("rows"),
            t,
            *images,
        )
        if column == 0:
            given += z_given
            images.append(z)
            krylov.append(u)
            coefficients.append(c)
            forward.fetch("rows", u)
            inverse.fetch("columns", u)
            links["forward"] = link(forward, inverse)
        state = rounds(forward, block, c, n, lambda _: product(forward, z))
        ev = state[4]
        if column == 0:
            inverse.fetch("blocks", state[1])
        operands, options = exchanged(forward, state)
        if column == 0:
            compose(inverse, state[0], block)
        basis = krylov if column == 0 else krylov + [u]
        count = len(basis)
        if last:
            out = shape(count * (count + 1), n, 128)
            gram = call(gram_kernel, out, big, *basis)
            p_own, p_near = forward.fetch("rows")
            _, block, received, cross, _ = state
            tail = operands[2 + len(received) :]
            z, z_given, rows, known = call(
                functools.partial(forward_last_kernel, column, *options),
                (
                    vectors,
                    shape(n, leaf),
                    shape(lax.axis_size("leaf"), SUMS, 2 * n),
                    shape(SUMS, n),
                ),
                4 * big,
                block,
                *received,
                cross,
                ev,
                p_own,
                p_near,
                *tail,
                gram,
                *totals,
                *krylov,
                u,
                z,
            )
            images.append(z)
            given.append(z_given)
            break
        part, sums, b = call(
            functools.partial(forward_part_kernel, count),
            (pair, shape(count, n, 128), shape(count, 2, n, rank)),
            (1 + count) * big,
            ev,
            *inverse.fetch("columns"),
            *forward.fetch("rows"),
            *basis,
        )
        outs = [pair, sums_shape, pair, block_shape] + ([] if column == 0 else [pair])
        d, t, c_next, block, *coefficient = call(
            functools.partial(forward_middle_end_kernel, column, *options),
            tuple(outs),
            4 * big,
            part,
            links["forward"],
            *operands,
            inverse.transfer,
            sums,
            b,
            *([] if column == 0 else [c]),
        )
        outs = [vectors] + ([] if column == 0 else [vectors, vectors, shape(n, leaf)])
        result = call(
            functools.partial(forward_image_kernel, column),
            tuple(outs),
            2 * big,
            d,
            ev,
            *forward.fetch("rows"),
            t,
            *([] if column == 0 else [u, z]),
        )
        w = result[0]
        if column > 0:
            krylov.append(result[1])
            images.append(result[2])
            given.append(result[3])
            coefficients.append(coefficient[0])
            totals.append(t)
        c = c_next

    got = lax.all_to_all(rows, "leaf", 0, 0)
    x, hess = call(
        answer_kernel,
        (shape(leaf, columns), shape(ITERS + 1, ITERS, columns)),
        big,
        got,
        known,
        with_partner(known),
        *[with_partner(z) for z in given],
        *images,
    )
    return (x, hess)


def solution(mesh):
    in_specs = (
        P("leaf", None),
        P("leaf", None, None),
        P("leaf", None, None),
        P("leaf", None, None),
        P(),
        P(),
        P("leaf", None, None),
        P("leaf", None, None),
        P("leaf", None, None),
        P(),
        P(),
    )
    out_specs = (P("leaf", None), P())
    return jax.shard_map(
        device_body, mesh=mesh, in_specs=in_specs, out_specs=out_specs, check_vma=False
    )
```
